32 devices in a mesh: sky: 4 (over x, core), tm: 8 (over z, y).
Axes of the slice: x: 2, y: 2, z: 4, core: 2. Of those that a mesh axis runs over, the one named last changes fastest.
Arguments:
- attitude: float32 [4, 8, 512], P(None, 'tm', 'sky'), may hold values from -6 to 6
- slot_time: float32 [262144], P(('sky', 'tm')), may hold values from -1 to 1
- slot_parallax: float32 [262144], P(('sky', 'tm')), may hold values from -1 to 1
- slot_observed: float32 [262144], P(('sky', 'tm')), may hold values from -6 to 6
- slot_phase: float32 [262144], P(('sky', 'tm')), may hold values from 0 to 1
- slot_knot: int32 [262144], P(('sky', 'tm')), may hold values from 0 to 508
- block_source: int32 [8192], P(('sky', 'tm')), may hold values from 0 to 63
- block_count: int32 [8192], P(('sky', 'tm')), may hold values from 1 to 32
- prior: float32 [5, 256], P(None, ('sky', 'tm')), may hold values from 0.5 to 4
Outputs:
- update: float32 [5, 256], P(None, ('sky', 'tm'))
The draws below stay inside these ranges and needn't reach their ends.
Inputs may be any that keep to these rules, and one draw needn't show every extreme that they name: The four knots from slot_knot on lie in the transit's time group of 512 knots. `block_source`: an index into the 64 sources of the block's own sky sector.
All inputs are finite; a program needn't handle non-finite values.
Results may differ from the reference program's by a relative error of at most 0.0003.
Values sent between devices are 32-bit elements; how exact they have to be, the bound alone decides.
A program may use at most 64 MiB of HBM per device.

```python
import math
import jax
import jax.numpy as jnp
from jax import lax

SLOTS = 32
PARAMS = 5
SRC_SKY = 64
SOURCES = 256
KNOTS_GROUP = 512
BLOCKS = 8192
TRANSITS = 262144
N_SKY = 4
N_TM = 8


def plant(values, key, low, high):
    longest = values.shape.index(max(values.shape))
    spots = []
    for shift in (0, 1):
        where = [jax.random.randint(jax.random.fold_in(key, axis), (), 0, length) for axis, length in enumerate(values.shape)]
        where[longest] = (where[longest] + shift) % values.shape[longest]
        spots.append(tuple(where))
    return values.at[spots[0]].set(low).at[spots[1]].set(high)


def shard_levels(stream_key, extent, cuts, low, top_value):
    loudness, own = 1.0, jax.random.fold_in(stream_key, 6)
    for dim, shards_of in cuts:
        heights = jnp.exp(jax.random.uniform(jax.random.fold_in(own, dim), (shards_of,), jnp.float32, low / len(cuts), top_value / len(cuts)))
        loudness = loudness * jnp.repeat(heights, extent[dim] // shards_of).reshape([-1 if axis == dim else 1 for axis in range(len(extent))])
    return loudness


def centred(key, shape, deviation, reach, shards=(), kind=jnp.bfloat16):
    values = deviation * jax.random.normal(key, shape, jnp.float32)
    if shards:
        values = values * shard_levels(key, shape, shards, -0.22, 0.18)
    return jnp.clip(values, -reach, reach).astype(kind)


def setup_inputs(seed: int = 0) -> dict:
    key_list = jax.random.split(jax.random.key(seed), 10)
    return {
        "attitude": centred(key_list[0], (4, N_TM, KNOTS_GROUP), 1.0, 6.0, ((1, 8), (2, 4)), jnp.float32),
        "slot_time": jnp.clip(jax.random.uniform(key_list[1], (TRANSITS,), jnp.float32, -1.0, 1.0) * shard_levels(key_list[1], (TRANSITS,), ((0, 32),), -0.4, 0.0), -1.0, 1.0),
        "slot_parallax": jnp.clip(jax.random.uniform(key_list[2], (TRANSITS,), jnp.float32, -1.0, 1.0) * shard_levels(key_list[2], (TRANSITS,), ((0, 32),), -0.4, 0.0), -1.0, 1.0),
        "slot_observed": centred(key_list[3], (TRANSITS,), 1.0, 6.0, ((0, 32),), jnp.float32),
        "slot_phase": jnp.clip(1.0 * jax.random.uniform(key_list[4], (TRANSITS,), jnp.float32) ** shard_levels(key_list[4], (TRANSITS,), ((0, 32),), -0.2, 0.2), 0.0, 1.0),
        "slot_knot": plant(jax.random.randint(key_list[5], (TRANSITS,), 0, KNOTS_GROUP - 3), jax.random.fold_in(key_list[5], 1), 0, (KNOTS_GROUP - 3) - 1).astype(jnp.int32),
        "block_source": plant(jax.random.randint(key_list[6], (BLOCKS,), 0, SRC_SKY), jax.random.fold_in(key_list[6], 1), 0, SRC_SKY - 1).astype(jnp.int32),
        "block_count": plant(jax.random.randint(key_list[7], (BLOCKS,), 1, SLOTS + 1), jax.random.fold_in(key_list[7], 1), 1, SLOTS).astype(jnp.int32),
        "prior": jnp.clip(jnp.exp(math.log(4.0) - 2.0794415 * jax.random.uniform(key_list[8], (PARAMS, SOURCES), jnp.float32) ** shard_levels(key_list[8], (PARAMS, SOURCES), ((1, 32),), -0.2, 0.2)), 0.5, 4.0),
    }


PAIR_LIST = [(i, j) for i in range(5) for j in range(i, 5)]

def block_sums(table, knot, phase, time, parallax, observed, count):
    weights = [(1.0 - phase) ** 3 / 6.0, (3.0 * phase ** 3 - 6.0 * phase ** 2 + 4.0) / 6.0, (-3.0 * phase ** 3 + 3.0 * phase ** 2 + 3.0 * phase + 1.0) / 6.0, phase ** 3 / 6.0]
    quat = weights[0][None, :] * table[:, knot]
    for i in range(1, 4):
        quat = quat + weights[i][None, :] * table[:, knot + i]
    cross = quat[0] * quat[0] + quat[1] * quat[1] - quat[2] * quat[2] - quat[3] * quat[3]
    along = 2.0 * (quat[1] * quat[2] + quat[0] * quat[3])
    tilt = 2.0 * (quat[1] * quat[3] - quat[0] * quat[2])
    design = [cross, along, parallax, time * cross, time * along]
    residual = observed - tilt
    rows = [design[i] * design[j] for i, j in PAIR_LIST] + [design[i] * residual for i in range(5)]
    stacked = jnp.stack(rows)
    blocks = count.shape[0]
    stacked = stacked.reshape(20, blocks, -1)
    live = (jnp.arange(stacked.shape[2], dtype=jnp.int32)[None, :] < count[:, None]).astype(stacked.dtype)
    return lax.optimization_barrier(jnp.sum(stacked * live[None], axis=2))

def solve_normals(normal, prior):
    entry = {}
    for index, pair in enumerate(PAIR_LIST):
        entry[pair[1], pair[0]] = normal[index]
    for i in range(5):
        entry[i, i] = entry[i, i] + prior[i]
    lower = {}
    for col in range(5):
        pivot = entry[col, col]
        for k in range(col):
            pivot = pivot - lower[col, k] * lower[col, k]
        root = jnp.sqrt(pivot)
        lower[col, col] = root
        for row in range(col + 1, 5):
            value = entry[row, col]
            for k in range(col):
                value = value - lower[row, k] * lower[col, k]
            lower[row, col] = value / root
    forward = []
    for i in range(5):
        value = normal[15 + i]
        for k in range(i):
            value = value - lower[i, k] * forward[k]
        forward.append(value / lower[i, i])
    result = [None] * 5
    for i in range(4, -1, -1):
        value = forward[i]
        for k in range(i + 1, 5):
            value = value - lower[k, i] * result[k]
        result[i] = value / lower[i, i]
    return jnp.stack(result)

def reference(attitude, slot_time, slot_parallax, slot_observed, slot_phase, slot_knot, block_source, block_count, prior):

    def per_slot(array):
        return array.reshape(N_SKY, N_TM, -1)
    prior_sky = jnp.transpose(prior.reshape(5, N_SKY, SRC_SKY), (1, 0, 2))

    def sector(items):
        knot, phase, time, parallax, observed, source, count, prior_here = items
        sums = jax.vmap(block_sums, in_axes=(1, 0, 0, 0, 0, 0, 0))(attitude, knot, phase, time, parallax, observed, count)
        flat = jnp.transpose(sums, (1, 0, 2)).reshape(20, -1)
        normal = jnp.zeros((20, SRC_SKY), jnp.float32).at[:, source.reshape(-1)].add(flat)
        return solve_normals(normal, prior_here)
    solved = lax.map(sector, (per_slot(slot_knot), per_slot(slot_phase), per_slot(slot_time), per_slot(slot_parallax), per_slot(slot_observed), per_slot(block_source), per_slot(block_count), prior_sky))
    return jnp.transpose(solved, (1, 0, 2)).reshape(5, SOURCES)
```

```python
import functools

import jax
import jax.numpy as jnp
from jax import lax
from jax.experimental import pallas as pl
from jax.experimental.pallas import tpu as pltpu
from jax.sharding import PartitionSpec as P

PAIR_LIST = [(i, j) for i in range(5) for j in range(i, 5)]
MESH = pl.DeviceIdType.MESH
LANES = 128
SUBS = 8
ROWS = 32


def lane_gather(row, index):
    wide = jnp.broadcast_to(row, index.shape)
    return jnp.take_along_axis(wide, index, axis=1, mode="promise_in_bounds")


def split2(value):
    high = value.astype(jnp.bfloat16)
    return high, (value - high.astype(jnp.float32)).astype(jnp.bfloat16)


def solve_rows(row, prior_row):
    entry = {}
    for i, j in PAIR_LIST:
        entry[j, i] = row(PLACE[i, j])
    for i in range(5):
        entry[i, i] = entry[i, i] + prior_row(i)
    right = [row(PLACE[i]) for i in range(5)]
    unit, inverse = {}, []
    for col in range(5):
        inv = 1.0 / entry[col, col]
        inverse.append(inv)
        for r in range(col + 1, 5):
            unit[r, col] = entry[r, col] * inv
        for r in range(col + 1, 5):
            for c in range(col + 1, r + 1):
                entry[r, c] = entry[r, c] - unit[r, col] * entry[c, col]
            right[r] = right[r] - unit[r, col] * right[col]
    result = [right[i] * inverse[i] for i in range(5)]
    for i in range(4, 0, -1):
        for k in range(i):
            result[k] = result[k] - unit[i, k] * result[i]
    return result


PLACE = {
    (0, 0): 0, (0, 1): 1, (0, 3): 2, (0, 4): 3, (1, 3): 3, (1, 1): 4, (1, 4): 5, (3, 3): 6, (3, 4): 7,
    (4, 4): 8, (0, 2): 9, (1, 2): 10, (2, 3): 11, (2, 4): 12, 0: 13, 1: 14, 2: 15,
    3: 16, 4: 17, (2, 2): 18,
}
SUMS = 19


def near_peers(tm, n_tm):
    if n_tm % 2 == 0 and n_tm <= 8:
        edges = [(tm + 1 - 2 * (tm % 2), None), (tm + 2, tm + 2 < n_tm), (tm - 2, tm >= 2)]
        return edges, n_tm // 2 - 1
    if n_tm & (n_tm - 1) == 0:
        bits = [1 << i for i in range(n_tm.bit_length() - 1)]
        return [(tm + bit * (1 - 2 * ((tm // bit) % 2)), None) for bit in bits], len(bits) - 1
    return [(lax.rem(tm + d, n_tm), None) for d in range(1, n_tm)], 0


def sky_peers(sky, n_sky):
    if n_sky & (n_sky - 1):
        sends = [(lax.rem(sky + d, n_sky), d) for d in range(1, n_sky)]
        return sends, [(lax.rem(sky + n_sky - d, n_sky), d) for d in range(1, n_sky)]
    core = sky % 2
    mate = sky + 1 - 2 * core
    sends, arrivals = [(mate, core)], [(mate, 1 - core)]
    for k in range(1, n_sky // 2):
        base = sky - core
        for bit in [1 << i for i in range(1, n_sky.bit_length())]:
            if 2 * k & bit:
                base = base + bit * (1 - 2 * ((sky // bit) % 2))
        sends += [(base, 2 * k + core), (base + 1, 2 * k + core)]
        arrivals += [(base + 1, 2 * k + 1), (base, 2 * k)]
    return sends, arrivals


def tell(semaphore, edges):
    for peer, exists in edges:

        def send(peer=peer):
            pl.semaphore_signal(semaphore, inc=1, device_id={"tm": peer}, device_id_type=MESH)

        if exists is None:
            send()
        else:
            pl.when(exists)(send)


def fold_subs(values, sub):
    values = list(values) + [jnp.zeros_like(values[0])] * (SUBS - len(values))
    values = [values[i] for i in (0, 4, 2, 6, 1, 5, 3, 7)]
    step = 1
    while step < SUBS:
        low = (sub // step) % 2 == 0
        half = len(values) // 2
        values = [
            jnp.where(low, a, b) + pltpu.roll(jnp.where(low, b, a), step, 0)
            for a, b in zip(values[:half], values[half:])
        ]
        step *= 2
    return values[0]


def kernel(
    n_sky, n_tm, span,
    attitude_hbm, time_hbm, parallax_hbm, observed_hbm, phase_hbm, knot_hbm,
    source_hbm, count_hbm, prior_hbm,
    out_ref, prior_ref,
    table, reals, ints, low, high, weight, masked, fact, quat, square, member, tiles, landed,
    real_sem, int_sem, prior_sem, own_sem, att_send, att_recv, sum_send, sum_recv, met,
):
    sky = lax.axis_index("sky")
    tm = lax.axis_index("tm")
    rows = time_hbm.shape[0]
    owned = tiles.shape[1]
    wide = source_hbm.shape[0]
    phase_v, time_v, parallax_v, observed_v = (reals.at[i] for i in range(4))
    knot_v = ints.at[:rows]
    source_v = ints.at[rows : rows + wide]
    count_v = ints.at[rows + wide :]
    sources = owned * n_tm
    segs = LANES // span
    fold = LANES // rows
    halves = segs // fold
    steps = span // SUBS

    own = pltpu.make_async_copy(attitude_hbm, table.at[sky], own_sem)
    own.start()
    barrier = pltpu.get_barrier_semaphore()
    sends, arrivals = sky_peers(sky, n_sky)
    for peer, _ in sends:
        pl.semaphore_signal(barrier, inc=1, device_id={"sky": peer}, device_id_type=MESH)
    edges, rounds = near_peers(tm, n_tm)
    degree = sum(1 if exists is None else exists.astype(jnp.int32) for _, exists in edges)
    tell(barrier, edges)
    for src, dst in ((source_hbm, source_v), (count_hbm, count_v), (knot_hbm, knot_v)):
        pltpu.make_async_copy(src, dst, int_sem).start()
    for i, src in enumerate((phase_hbm, time_hbm, parallax_hbm, observed_hbm)):
        pltpu.make_async_copy(src, reals.at[i], real_sem).start()
    prior_copy = pltpu.make_async_copy(prior_hbm, prior_ref, prior_sem)
    prior_copy.start()

    tiles[...] = jnp.zeros_like(tiles)

    own.wait()
    pl.semaphore_wait(barrier, n_sky - 1 + degree)
    for peer, there in sends:
        pltpu.make_async_remote_copy(
            src_ref=table.at[sky],
            dst_ref=table.at[sky],
            send_sem=att_send,
            recv_sem=att_recv.at[there],
            device_id={"sky": peer},
            device_id_type=MESH,
        ).start()
    if rounds:
        tell(met.at[0], edges)

    pltpu.make_async_copy(ints, ints, int_sem).wait()
    lane = lax.broadcasted_iota(jnp.int32, (SUBS, LANES), 1)
    sub = lax.broadcasted_iota(jnp.int32, (SUBS, LANES), 0)
    count = []
    which = lax.broadcasted_iota(jnp.int32, (sources, LANES), 0)
    for h in range(halves):
        block = (lane % rows) * segs + h * fold + lane // rows

        def of_block(ref):
            got = lane_gather(ref[0:1, :], block % LANES)
            for c in range(1, wide):
                got = jnp.where(block // LANES == c, lane_gather(ref[c : c + 1, :], block % LANES), got)
            return got

        count.append(of_block(count_v))
        hit = jnp.broadcast_to(of_block(source_v)[0:1, :], (sources, LANES)) == which
        one = jnp.where(hit, 1.0, 0.0).astype(jnp.bfloat16)
        for k in range(2):
            at = (k * halves + h) * LANES
            member[:, at : at + LANES] = one

    def turn(value):
        parts = [value] + [pltpu.roll(value, LANES - e * span, 1) for e in range(1, fold)]
        turned = jnp.transpose(jnp.concatenate(parts, axis=0))
        return [turned[h * fold * span : h * fold * span + span, :] for h in range(halves)]

    for h, knot in enumerate(turn(knot_v[...])):
        at = slice(h * span, h * span + span)
        low[at, :] = knot % LANES
        high[at, :] = knot // LANES

    pltpu.make_async_copy(reals, reals, real_sem).wait()
    turned = [turn(ref[...]) for ref in (phase_v, time_v, parallax_v, observed_v)]
    for h in range(halves):
        at = slice(h * span, h * span + span)
        u, time, parallax, observed = (t[h] for t in turned)
        slot = lax.broadcasted_iota(jnp.int32, (span, LANES), 0)
        live = slot < jnp.broadcast_to(count[h][0:1, :], (span, LANES))
        u2, v = u * u, 1.0 - u
        u3 = u2 * u
        spline = (
            v * v * v * (1.0 / 6.0),
            0.5 * u3 - u2 + (2.0 / 3.0),
            0.5 * (u + u2 - u3) + (1.0 / 6.0),
            u3 * (1.0 / 6.0),
        )
        for i in range(4):
            weight[i, at, :] = jnp.where(live, spline[i], 0.0)
        parallax = jnp.where(live, parallax, 0.0)
        fact[0, at, :] = time
        fact[1, at, :] = time * time
        fact[2, at, :] = parallax
        fact[3, at, :] = parallax * time
        fact[4, at, :] = observed
        both = parallax * parallax
        total = both[:SUBS]
        for g in range(1, steps):
            total = total + both[g * SUBS : (g + 1) * SUBS]
        square[h] = total

    if rounds:
        pl.semaphore_wait(met.at[0], degree)
        if rounds > 1:
            tell(met.at[1], edges)

    per = table.shape[2] // LANES

    def mask_weights(chunk):
        lows, highs = low[...], high[...]
        for i in range(4):
            there = highs + (lows >= LANES - i).astype(jnp.int32) if i else highs
            masked[i] = jnp.where(there == chunk, weight[i], 0.0)

    def rows_of(source, p):
        here = table[source, :, p * LANES : (p + 1) * LANES]
        return [here] + [pltpu.roll(here, LANES - i, 1) for i in range(1, 4)]

    def gather(shifted, v, carry):
        at = slice(v * SUBS, v * SUBS + SUBS)
        index = low[at, :]
        scale = [masked[i, at, :] for i in range(4)]
        got = []
        for m in range(4):
            value = carry[m] if carry else None
            for i in range(4):
                term = lane_gather(shifted[i][m : m + 1, :], index) * scale[i]
                value = term if value is None else value + term
            got.append(value)
        return got

    pieces = [(sky, None, p) for p in range(per)]
    for source, here in arrivals:
        pieces += [(source, here if p == 0 else None, p) for p in range(per)]
    for n, (source, here, p) in enumerate(pieces):
        mask_weights(source * per + p)
        if n == 1:
            for step in range(2, rounds):
                pl.semaphore_wait(met.at[step - 1], degree)
                tell(met.at[step], edges)
        if here is not None:
            arrived = table.at[source]
            pltpu.make_async_copy(arrived, arrived, att_recv.at[here]).wait()
        shifted = rows_of(source, p)
        if n + 1 < len(pieces):
            for v in range(rows // SUBS):
                at = slice(v * SUBS, v * SUBS + SUBS)
                got = gather(shifted, v, [quat[m, at, :] for m in range(4)] if n else None)
                for m in range(4):
                    quat[m, at, :] = got[m]

    stacked = []
    for h in range(halves):
        sums = None
        for g in range(steps):
            v = h * steps + g
            at = slice(v * SUBS, v * SUBS + SUBS)
            carry = [quat[m, at, :] for m in range(4)] if len(pieces) > 1 else None
            q0, q1, q2, q3 = gather(shifted, v, carry)
            cross = (q0 * q0 + q1 * q1) - (q2 * q2 + q3 * q3)
            along = 2.0 * (q1 * q2 + q0 * q3)
            tilt = 2.0 * (q1 * q3 - q0 * q2)
            t, tt, p, tp, o = (fact[i, at, :] for i in range(5))
            rest = o - tilt
            cc, ca, aa = cross * cross, cross * along, along * along
            cr, ar = cross * rest, along * rest
            new = {
                (0, 0): cc, (0, 1): ca, (0, 3): t * cc, (0, 4): t * ca, (1, 1): aa, (1, 4): t * aa,
                (3, 3): tt * cc, (3, 4): tt * ca, (4, 4): tt * aa,
                (0, 2): p * cross, (1, 2): p * along, (2, 3): tp * cross, (2, 4): tp * along,
                0: cr, 1: ar, 2: p * rest, 3: t * cr, 4: t * ar,
            }
            sums = new if sums is None else {key: sums[key] + new[key] for key in new}
        sums[2, 2] = square[h]
        line = [sums[key] for key in sorted(sums, key=lambda key: PLACE[key])]
        groups = [fold_subs(line[i : i + SUBS], sub) for i in range(0, SUMS, SUBS)]
        groups += [jnp.zeros_like(groups[0])] * (ROWS // SUBS - len(groups))
        stacked.append(jnp.concatenate(groups, axis=0))
    split = [split2(value) for value in stacked]
    packed = jnp.concatenate([s[k] for k in range(2) for s in split], axis=1)
    normal = lax.dot_general(
        member[...], packed, (((1,), (1,)), ((), ())), preferred_element_type=jnp.float32
    )
    tiles[:, :, :ROWS] = normal.reshape(n_tm, owned, ROWS)
    if rounds:
        pl.semaphore_wait(met.at[rounds - 1], degree)

    for d in range(1, n_tm):
        peer = lax.rem(tm + d, n_tm)
        pltpu.make_async_remote_copy(
            src_ref=tiles.at[peer],
            dst_ref=landed.at[d - 1],
            send_sem=sum_send,
            recv_sem=sum_recv,
            device_id={"tm": peer},
            device_id_type=MESH,
        ).start()
    prior_copy.wait()
    others = table.at[: n_sky - 1]
    pltpu.make_async_copy(others, others, att_send).wait()
    total = tiles[tm]
    pltpu.make_async_copy(landed, landed, sum_recv).wait()
    for d in range(1, n_tm):
        total = total + landed[d - 1]
    out_ref[...] = total
    pltpu.make_async_copy(landed, landed, sum_send).wait()


def solve_kernel(total_ref, prior_ref, out_ref, turned):
    turned[...] = jnp.transpose(total_ref[...])[:ROWS]
    result = solve_rows(lambda i: turned[i : i + 1, :], lambda i: prior_ref[i : i + 1, :])
    for i in range(5):
        out_ref[i : i + 1, :] = result[i]


def on_device(n_sky, n_tm, attitude, time, parallax, observed, phase, knot, source, count, prior):
    slots, blocks, owned = time.shape[0], source.shape[0], prior.shape[1]
    knots = attitude.shape[2]
    rows = slots // LANES
    span = slots // blocks
    sources = owned * n_tm
    shape = (rows, LANES)
    vmem = pltpu.VMEM
    f32, i32, bf16 = jnp.float32, jnp.int32, jnp.bfloat16
    halves = (LANES // span) // (LANES // rows)
    total, prior_near = pl.pallas_call(
        functools.partial(kernel, n_sky, n_tm, span),
        out_shape=(pltpu.VMEM((owned, LANES), f32), pltpu.VMEM(prior.shape, f32)),
        in_specs=[pl.BlockSpec(memory_space=pl.ANY)] * 9,
        out_specs=(pl.BlockSpec(memory_space=pltpu.VMEM),) * 2,
        scratch_shapes=[
            vmem((n_sky, 4, knots), f32),
            vmem((4,) + shape, f32),
            vmem((rows + 2 * (blocks // LANES), LANES), i32),
            vmem(shape, i32),
            vmem(shape, i32),
            vmem((4,) + shape, f32),
            vmem((4,) + shape, f32),
            vmem((5,) + shape, f32),
            vmem((4,) + shape, f32),
            vmem((halves, SUBS, LANES), f32),
            vmem((sources, 2 * blocks), bf16),
            vmem((n_tm, owned, LANES), f32),
            vmem((n_tm - 1, owned, LANES), f32),
        ]
        + [pltpu.SemaphoreType.DMA] * 5
        + [pltpu.SemaphoreType.DMA((n_sky,))]
        + [pltpu.SemaphoreType.DMA] * 2
        + [pltpu.SemaphoreType.REGULAR((max(1, near_peers(0, n_tm)[1]),))],
        compiler_params=pltpu.CompilerParams(collective_id=0, has_side_effects=True),
    )(
        attitude.reshape(4, knots),
        time.reshape(shape),
        parallax.reshape(shape),
        observed.reshape(shape),
        phase.reshape(shape),
        knot.reshape(shape),
        source.reshape(blocks // LANES, LANES),
        count.reshape(blocks // LANES, LANES),
        prior,
    )
    return pl.pallas_call(
        solve_kernel,
        out_shape=jax.ShapeDtypeStruct(prior.shape, f32),
        in_specs=[pl.BlockSpec(memory_space=pltpu.VMEM)] * 2,
        scratch_shapes=[vmem((ROWS, owned), f32)],
    )(
        pltpu.with_memory_space_constraint(total, pltpu.VMEM),
        pltpu.with_memory_space_constraint(prior_near, pltpu.VMEM),
    )


def solution(mesh):
    slot = P(("sky", "tm"))
    in_specs = (P(None, "tm", "sky"),) + (slot,) * 7 + (P(None, ("sky", "tm")),)
    return jax.shard_map(
        functools.partial(on_device, mesh.shape["sky"], mesh.shape["tm"]),
        mesh=mesh,
        in_specs=in_specs,
        out_specs=P(None, ("sky", "tm")),
        check_vma=False,
    )
```

```python
import functools

import jax
import jax.numpy as jnp
from jax import lax
from jax.experimental import pallas as pl
from jax.experimental.pallas import tpu as pltpu
from jax.sharding import PartitionSpec as P

PAIR_LIST = [(i, j) for i in range(5) for j in range(i, 5)]
MESH = pl.DeviceIdType.MESH
LANES = 128
SUBS = 8
ROWS = 32


def lane_gather(row, index):
    wide = jnp.broadcast_to(row, index.shape)
    return jnp.take_along_axis(wide, index, axis=1, mode="promise_in_bounds")


def split2(value):
    high = value.astype(jnp.bfloat16)
    return high, (value - high.astype(jnp.float32)).astype(jnp.bfloat16)


def solve_rows(row, prior_row):
    entry = {}
    for i, j in PAIR_LIST:
        entry[j, i] = row(PLACE[i, j])
    for i in range(5):
        entry[i, i] = entry[i, i] + prior_row(i)
    right = [row(PLACE[i]) for i in range(5)]
    unit, inverse = {}, []
    for col in range(5):
        inv = 1.0 / entry[col, col]
        inverse.append(inv)
        for r in range(col + 1, 5):
            unit[r, col] = entry[r, col] * inv
        for r in range(col + 1, 5):
            for c in range(col + 1, r + 1):
                entry[r, c] = entry[r, c] - unit[r, col] * entry[c, col]
            right[r] = right[r] - unit[r, col] * right[col]
    result = [right[i] * inverse[i] for i in range(5)]
    for i in range(4, 0, -1):
        for k in range(i):
            result[k] = result[k] - unit[i, k] * result[i]
    return result


PLACE = {
    (0, 0): 0, (0, 1): 1, (0, 3): 2, (0, 4): 3, (1, 3): 3, (1, 1): 4, (1, 4): 5, (3, 3): 6, (3, 4): 7,
    (4, 4): 8, (0, 2): 9, (1, 2): 10, (2, 3): 11, (2, 4): 12, 0: 13, 1: 14, 2: 15,
    3: 16, 4: 17, (2, 2): 18,
}
SUMS = 19


def rank_of(tm, n_tm):
    return tm // 2 + tm % 2 if n_tm % 2 == 0 and n_tm <= 8 else tm


def sky_peers(sky, n_sky):
    if n_sky & (n_sky - 1):
        sends = [(lax.rem(sky + d, n_sky), d) for d in range(1, n_sky)]
        return sends, [(lax.rem(sky + n_sky - d, n_sky), d) for d in range(1, n_sky)]
    core = sky % 2
    mate = sky + 1 - 2 * core
    sends, arrivals = [(mate, core)], [(mate, 1 - core)]
    for k in range(1, n_sky // 2):
        base = sky - core
        for bit in [1 << i for i in range(1, n_sky.bit_length())]:
            if 2 * k & bit:
                base = base + bit * (1 - 2 * ((sky // bit) % 2))
        sends += [(base, 2 * k + core), (base + 1, 2 * k + core)]
        arrivals += [(base + 1, 2 * k + 1), (base, 2 * k)]
    return sends, arrivals


def tell(semaphore, peer, exists):
    @pl.when(exists)
    def _():
        pl.semaphore_signal(semaphore, inc=1, device_id={"tm": peer}, device_id_type=MESH)


def fold_subs(values, sub):
    values = list(values) + [jnp.zeros_like(values[0])] * (SUBS - len(values))
    values = [values[i] for i in (0, 4, 2, 6, 1, 5, 3, 7)]
    step = 1
    while step < SUBS:
        low = (sub // step) % 2 == 0
        half = len(values) // 2
        values = [
            jnp.where(low, a, b) + pltpu.roll(jnp.where(low, b, a), step, 0)
            for a, b in zip(values[:half], values[half:])
        ]
        step *= 2
    return values[0]


def kernel(
    n_sky, n_tm, span,
    attitude_hbm, time_hbm, parallax_hbm, observed_hbm, phase_hbm, knot_hbm,
    source_hbm, count_hbm, prior_hbm,
    out_ref, prior_ref,
    table, reals, ints, low, high, weight, masked, fact, quat, square, member, tiles, landed,
    real_sem, int_sem, prior_sem, own_sem, att_send, att_recv, sum_send, sum_recv, met,
):
    sky = lax.axis_index("sky")
    tm = lax.axis_index("tm")
    rows = time_hbm.shape[0]
    owned = tiles.shape[1]
    wide = source_hbm.shape[0]
    phase_v, time_v, parallax_v, observed_v = (reals.at[i] for i in range(4))
    knot_v = ints.at[:rows]
    source_v = ints.at[rows : rows + wide]
    count_v = ints.at[rows + wide :]
    sources = owned * n_tm
    segs = LANES // span
    fold = LANES // rows
    halves = segs // fold
    steps = span // SUBS

    own = pltpu.make_async_copy(attitude_hbm, table.at[sky], own_sem)
    own.start()
    barrier = pltpu.get_barrier_semaphore()
    sends, arrivals = sky_peers(sky, n_sky)
    for peer, _ in sends:
        pl.semaphore_signal(barrier, inc=1, device_id={"sky": peer}, device_id_type=MESH)
    for src, dst in ((source_hbm, source_v), (count_hbm, count_v), (knot_hbm, knot_v)):
        pltpu.make_async_copy(src, dst, int_sem).start()
    for i, src in enumerate((phase_hbm, time_hbm, parallax_hbm, observed_hbm)):
        pltpu.make_async_copy(src, reals.at[i], real_sem).start()
    prior_copy = pltpu.make_async_copy(prior_hbm, prior_ref, prior_sem)
    prior_copy.start()
    rank = rank_of(tm, n_tm)
    ranks = [rank_of(peer, n_tm) for peer in range(n_tm)]
    below = sum((rank > other).astype(jnp.int32) for other in ranks)
    above = sum((rank < other).astype(jnp.int32) for other in ranks)
    for peer, other in enumerate(ranks):
        tell(barrier, peer, rank < other)

    tiles[...] = jnp.zeros_like(tiles)

    own.wait()
    pl.semaphore_wait(barrier, n_sky - 1 + below)
    for peer, there in sends:
        pltpu.make_async_remote_copy(
            src_ref=table.at[sky],
            dst_ref=table.at[sky],
            send_sem=att_send,
            recv_sem=att_recv.at[there],
            device_id={"sky": peer},
            device_id_type=MESH,
        ).start()
    for peer, other in enumerate(ranks):
        tell(met, peer, rank > other)

    pltpu.make_async_copy(ints, ints, int_sem).wait()
    lane = lax.broadcasted_iota(jnp.int32, (SUBS, LANES), 1)
    sub = lax.broadcasted_iota(jnp.int32, (SUBS, LANES), 0)
    count = []
    which = lax.broadcasted_iota(jnp.int32, (sources, LANES), 0)
    for h in range(halves):
        block = (lane % rows) * segs + h * fold + lane // rows

        def of_block(ref):
            got = lane_gather(ref[0:1, :], block % LANES)
            for c in range(1, wide):
                got = jnp.where(block // LANES == c, lane_gather(ref[c : c + 1, :], block % LANES), got)
            return got

        count.append(of_block(count_v))
        hit = jnp.broadcast_to(of_block(source_v)[0:1, :], (sources, LANES)) == which
        one = jnp.where(hit, 1.0, 0.0).astype(jnp.bfloat16)
        for k in range(2):
            at = (k * halves + h) * LANES
            member[:, at : at + LANES] = one

    def turn(value):
        parts = [value] + [pltpu.roll(value, LANES - e * span, 1) for e in range(1, fold)]
        turned = jnp.transpose(jnp.concatenate(parts, axis=0))
        return [turned[h * fold * span : h * fold * span + span, :] for h in range(halves)]

    for h, knot in enumerate(turn(knot_v[...])):
        at = slice(h * span, h * span + span)
        low[at, :] = knot % LANES
        high[at, :] = knot // LANES

    pltpu.make_async_copy(reals, reals, real_sem).wait()
    turned = [turn(ref[...]) for ref in (phase_v, time_v, parallax_v, observed_v)]
    for h in range(halves):
        at = slice(h * span, h * span + span)
        u, time, parallax, observed = (t[h] for t in turned)
        slot = lax.broadcasted_iota(jnp.int32, (span, LANES), 0)
        live = slot < jnp.broadcast_to(count[h][0:1, :], (span, LANES))
        u2, v = u * u, 1.0 - u
        u3 = u2 * u
        spline = (
            v * v * v * (1.0 / 6.0),
            0.5 * u3 - u2 + (2.0 / 3.0),
            0.5 * (u + u2 - u3) + (1.0 / 6.0),
            u3 * (1.0 / 6.0),
        )
        for i in range(4):
            weight[i, at, :] = jnp.where(live, spline[i], 0.0)
        parallax = jnp.where(live, parallax, 0.0)
        fact[0, at, :] = time
        fact[1, at, :] = time * time
        fact[2, at, :] = parallax
        fact[3, at, :] = parallax * time
        fact[4, at, :] = observed
        both = parallax * parallax
        total = both[:SUBS]
        for g in range(1, steps):
            total = total + both[g * SUBS : (g + 1) * SUBS]
        square[h] = total

    per = table.shape[2] // LANES

    def mask_weights(chunk):
        lows, highs = low[...], high[...]
        for i in range(4):
            there = highs + (lows >= LANES - i).astype(jnp.int32) if i else highs
            masked[i] = jnp.where(there == chunk, weight[i], 0.0)

    def rows_of(source, p):
        here = table[source, :, p * LANES : (p + 1) * LANES]
        return [here] + [pltpu.roll(here, LANES - i, 1) for i in range(1, 4)]

    def gather(shifted, v, carry):
        at = slice(v * SUBS, v * SUBS + SUBS)
        index = low[at, :]
        scale = [masked[i, at, :] for i in range(4)]
        got = []
        for m in range(4):
            value = carry[m] if carry else None
            for i in range(4):
                term = lane_gather(shifted[i][m : m + 1, :], index) * scale[i]
                value = term if value is None else value + term
            got.append(value)
        return got

    pieces = [(sky, None, p) for p in range(per)]
    for source, here in arrivals:
        pieces += [(source, here if p == 0 else None, p) for p in range(per)]
    for n, (source, here, p) in enumerate(pieces):
        mask_weights(source * per + p)
        if here is not None:
            arrived = table.at[source]
            pltpu.make_async_copy(arrived, arrived, att_recv.at[here]).wait()
        shifted = rows_of(source, p)
        if n + 1 < len(pieces):
            for v in range(rows // SUBS):
                at = slice(v * SUBS, v * SUBS + SUBS)
                got = gather(shifted, v, [quat[m, at, :] for m in range(4)] if n else None)
                for m in range(4):
                    quat[m, at, :] = got[m]

    stacked = []
    for h in range(halves):
        sums = None
        for g in range(steps):
            v = h * steps + g
            at = slice(v * SUBS, v * SUBS + SUBS)
            carry = [quat[m, at, :] for m in range(4)] if len(pieces) > 1 else None
            q0, q1, q2, q3 = gather(shifted, v, carry)
            cross = (q0 * q0 + q1 * q1) - (q2 * q2 + q3 * q3)
            along = 2.0 * (q1 * q2 + q0 * q3)
            tilt = 2.0 * (q1 * q3 - q0 * q2)
            t, tt, p, tp, o = (fact[i, at, :] for i in range(5))
            rest = o - tilt
            cc, ca, aa = cross * cross, cross * along, along * along
            cr, ar = cross * rest, along * rest
            new = {
                (0, 0): cc, (0, 1): ca, (0, 3): t * cc, (0, 4): t * ca, (1, 1): aa, (1, 4): t * aa,
                (3, 3): tt * cc, (3, 4): tt * ca, (4, 4): tt * aa,
                (0, 2): p * cross, (1, 2): p * along, (2, 3): tp * cross, (2, 4): tp * along,
                0: cr, 1: ar, 2: p * rest, 3: t * cr, 4: t * ar,
            }
            sums = new if sums is None else {key: sums[key] + new[key] for key in new}
        sums[2, 2] = square[h]
        line = [sums[key] for key in sorted(sums, key=lambda key: PLACE[key])]
        groups = [fold_subs(line[i : i + SUBS], sub) for i in range(0, SUMS, SUBS)]
        groups += [jnp.zeros_like(groups[0])] * (ROWS // SUBS - len(groups))
        stacked.append(jnp.concatenate(groups, axis=0))
    split = [split2(value) for value in stacked]
    packed = jnp.concatenate([s[k] for k in range(2) for s in split], axis=1)
    normal = lax.dot_general(
        member[...], packed, (((1,), (1,)), ((), ())), preferred_element_type=jnp.float32
    )
    tiles[:, :, :ROWS] = normal.reshape(n_tm, owned, ROWS)

    @pl.when(above > 0)
    def _():
        pl.semaphore_wait(met, above)

    for d in range(1, n_tm):
        peer = lax.rem(tm + d, n_tm)
        pltpu.make_async_remote_copy(
            src_ref=tiles.at[peer],
            dst_ref=landed.at[d - 1],
            send_sem=sum_send,
            recv_sem=sum_recv,
            device_id={"tm": peer},
            device_id_type=MESH,
        ).start()
    prior_copy.wait()
    others = table.at[: n_sky - 1]
    pltpu.make_async_copy(others, others, att_send).wait()
    total = tiles[tm]
    pltpu.make_async_copy(landed, landed, sum_recv).wait()
    for d in range(1, n_tm):
        total = total + landed[d - 1]
    out_ref[...] = total
    pltpu.make_async_copy(landed, landed, sum_send).wait()


def solve_kernel(total_ref, prior_ref, out_ref, turned):
    turned[...] = jnp.transpose(total_ref[...])[:ROWS]
    result = solve_rows(lambda i: turned[i : i + 1, :], lambda i: prior_ref[i : i + 1, :])
    for i in range(5):
        out_ref[i : i + 1, :] = result[i]


def on_device(n_sky, n_tm, attitude, time, parallax, observed, phase, knot, source, count, prior):
    slots, blocks, owned = time.shape[0], source.shape[0], prior.shape[1]
    knots = attitude.shape[2]
    rows = slots // LANES
    span = slots // blocks
    sources = owned * n_tm
    shape = (rows, LANES)
    vmem = pltpu.VMEM
    f32, i32, bf16 = jnp.float32, jnp.int32, jnp.bfloat16
    halves = (LANES // span) // (LANES // rows)
    total, prior_near = pl.pallas_call(
        functools.partial(kernel, n_sky, n_tm, span),
        out_shape=(pltpu.VMEM((owned, LANES), f32), pltpu.VMEM(prior.shape, f32)),
        in_specs=[pl.BlockSpec(memory_space=pl.ANY)] * 9,
        out_specs=(pl.BlockSpec(memory_space=pltpu.VMEM),) * 2,
        scratch_shapes=[
            vmem((n_sky, 4, knots), f32),
            vmem((4,) + shape, f32),
            vmem((rows + 2 * (blocks // LANES), LANES), i32),
            vmem(shape, i32),
            vmem(shape, i32),
            vmem((4,) + shape, f32),
            vmem((4,) + shape, f32),
            vmem((5,) + shape, f32),
            vmem((4,) + shape, f32),
            vmem((halves, SUBS, LANES), f32),
            vmem((sources, 2 * blocks), bf16),
            vmem((n_tm, owned, LANES), f32),
            vmem((n_tm - 1, owned, LANES), f32),
        ]
        + [pltpu.SemaphoreType.DMA] * 5
        + [pltpu.SemaphoreType.DMA((n_sky,))]
        + [pltpu.SemaphoreType.DMA] * 2
        + [pltpu.SemaphoreType.REGULAR],
        compiler_params=pltpu.CompilerParams(collective_id=0, has_side_effects=True),
    )(
        attitude.reshape(4, knots),
        time.reshape(shape),
        parallax.reshape(shape),
        observed.reshape(shape),
        phase.reshape(shape),
        knot.reshape(shape),
        source.reshape(blocks // LANES, LANES),
        count.reshape(blocks // LANES, LANES),
        prior,
    )
    return pl.pallas_call(
        solve_kernel,
        out_shape=jax.ShapeDtypeStruct(prior.shape, f32),
        in_specs=[pl.BlockSpec(memory_space=pltpu.VMEM)] * 2,
        scratch_shapes=[vmem((ROWS, owned), f32)],
    )(
        pltpu.with_memory_space_constraint(total, pltpu.VMEM),
        pltpu.with_memory_space_constraint(prior_near, pltpu.VMEM),
    )


def solution(mesh):
    slot = P(("sky", "tm"))
    in_specs = (P(None, "tm", "sky"),) + (slot,) * 7 + (P(None, ("sky", "tm")),)
    return jax.shard_map(
        functools.partial(on_device, mesh.shape["sky"], mesh.shape["tm"]),
        mesh=mesh,
        in_specs=in_specs,
        out_specs=P(None, ("sky", "tm")),
        check_vma=False,
    )
```

```python
import functools

import jax
import jax.numpy as jnp
from jax import lax
from jax.experimental import pallas as pl
from jax.experimental.pallas import tpu as pltpu
from jax.sharding import PartitionSpec as P

PAIR_LIST = [(i, j) for i in range(5) for j in range(i, 5)]
MESH = pl.DeviceIdType.MESH
LANES = 128
SUBS = 8
ROWS = 32


def lane_gather(row, index):
    wide = jnp.broadcast_to(row, index.shape)
    return jnp.take_along_axis(wide, index, axis=1, mode="promise_in_bounds")


def split2(value):
    high = value.astype(jnp.bfloat16)
    return high, (value - high.astype(jnp.float32)).astype(jnp.bfloat16)


def solve_rows(row, prior_row):
    entry = {}
    for i, j in PAIR_LIST:
        entry[j, i] = row(PLACE[i, j])
    for i in range(5):
        entry[i, i] = entry[i, i] + prior_row(i)
    right = [row(PLACE[i]) for i in range(5)]
    unit, inverse = {}, []
    for col in range(5):
        inv = 1.0 / entry[col, col]
        inverse.append(inv)
        for r in range(col + 1, 5):
            unit[r, col] = entry[r, col] * inv
        for r in range(col + 1, 5):
            for c in range(col + 1, r + 1):
                entry[r, c] = entry[r, c] - unit[r, col] * entry[c, col]
            right[r] = right[r] - unit[r, col] * right[col]
    result = [right[i] * inverse[i] for i in range(5)]
    for i in range(4, 0, -1):
        for k in range(i):
            result[k] = result[k] - unit[i, k] * result[i]
    return result


PLACE = {
    (0, 0): 0, (0, 1): 1, (0, 3): 2, (0, 4): 3, (1, 3): 3, (1, 1): 4, (1, 4): 5, (3, 3): 6, (3, 4): 7,
    (4, 4): 8, (0, 2): 9, (1, 2): 10, (2, 3): 11, (2, 4): 12, 0: 13, 1: 14, 2: 15,
    3: 16, 4: 17, (2, 2): 18,
}
SUMS = 19


def orders(tm, n_tm):
    if n_tm % 2 == 0 and n_tm <= 8:

        def order(peer):
            up, across = peer // 2, peer % 2
            earlier = jnp.logical_and(tm // 2 >= up, tm % 2 >= across)
            later = jnp.logical_and(tm // 2 <= up, tm % 2 <= across)
            return jnp.logical_and(earlier, tm != peer), jnp.logical_and(later, tm != peer)
    else:

        def order(peer):
            return tm > peer, tm < peer

    return [(peer, *order(peer)) for peer in range(n_tm)]


def sky_peers(sky, n_sky):
    if n_sky & (n_sky - 1):
        sends = [(lax.rem(sky + d, n_sky), d - 1) for d in range(1, n_sky)]
        return sends, [(lax.rem(sky + n_sky - d, n_sky), d - 1) for d in range(1, n_sky)]
    core = sky % 2
    mate = sky + 1 - 2 * core
    sends, arrivals = [], [(mate, 0)]
    for k in range(1, n_sky // 2):
        base = sky - core
        for bit in [1 << i for i in range(1, n_sky.bit_length())]:
            if 2 * k & bit:
                base = base + bit * (1 - 2 * ((sky // bit) % 2))
        sends += [(base, 2 * k - 1 + core), (base + 1, 2 * k - 1 + core)]
        arrivals += [(base + 1, 2 * k), (base, 2 * k - 1)]
    return sends + [(mate, 0)], arrivals


def tell(semaphore, peer, exists):
    @pl.when(exists)
    def _():
        pl.semaphore_signal(semaphore, inc=1, device_id={"tm": peer}, device_id_type=MESH)


def fold_subs(values, sub):
    values = list(values) + [jnp.zeros_like(values[0])] * (SUBS - len(values))
    values = [values[i] for i in (0, 4, 2, 6, 1, 5, 3, 7)]
    step = 1
    while step < SUBS:
        low = (sub // step) % 2 == 0
        half = len(values) // 2
        values = [
            jnp.where(low, a, b) + pltpu.roll(jnp.where(low, b, a), step, 0)
            for a, b in zip(values[:half], values[half:])
        ]
        step *= 2
    return values[0]


def kernel(
    n_sky, n_tm, span,
    attitude_hbm, time_hbm, parallax_hbm, observed_hbm, phase_hbm, knot_hbm,
    source_hbm, count_hbm, prior_hbm,
    out_ref,
    mine, table, reals, ints, low, high, weight, masked, fact, quat, square, member, tiles, landed,
    real_sem, int_sem, send_sem, att_recv, sum_recv, met, prior_ref, flat, packed,
):
    own = pltpu.make_async_copy(attitude_hbm, mine, send_sem)
    own.start()
    sky = lax.axis_index("sky")
    tm = lax.axis_index("tm")
    rows = time_hbm.shape[0]
    owned = tiles.shape[1]
    wide = source_hbm.shape[0]
    phase_v, time_v, parallax_v, observed_v = (reals.at[i] for i in range(4))
    knot_v = ints.at[:rows]
    source_v = ints.at[rows : rows + wide]
    count_v = ints.at[rows + wide :]
    sources = owned * n_tm
    segs = LANES // span
    fold = LANES // rows
    halves = segs // fold
    steps = span // SUBS

    barrier = pltpu.get_barrier_semaphore()
    sends, arrivals = sky_peers(sky, n_sky)
    for peer, _ in sends:
        pl.semaphore_signal(barrier, inc=1, device_id={"sky": peer}, device_id_type=MESH)
    for src, dst in ((source_hbm, source_v), (count_hbm, count_v), (knot_hbm, knot_v)):
        pltpu.make_async_copy(src, dst, int_sem).start()
    for i, src in enumerate((phase_hbm, time_hbm, parallax_hbm, observed_hbm)):
        pltpu.make_async_copy(src, reals.at[i], real_sem).start()
    peers = orders(tm, n_tm)
    below = sum(earlier.astype(jnp.int32) for _, earlier, _ in peers)
    above = sum(later.astype(jnp.int32) for _, _, later in peers)
    for peer, _, later in peers:
        tell(barrier, peer, later)

    tiles[...] = jnp.zeros_like(tiles)

    own.wait()
    pl.semaphore_wait(barrier, n_sky - 1 + below)
    for peer, there in sends:
        pltpu.make_async_remote_copy(
            src_ref=mine,
            dst_ref=table.at[sky],
            send_sem=send_sem,
            recv_sem=att_recv.at[there],
            device_id={"sky": peer},
            device_id_type=MESH,
        ).start()
    for peer, earlier, _ in peers:
        tell(met, peer, earlier)

    pltpu.make_async_copy(ints, ints, int_sem).wait()
    prior_copy = pltpu.make_async_copy(prior_hbm, prior_ref, int_sem)
    prior_copy.start()
    lane = lax.broadcasted_iota(jnp.int32, (SUBS, LANES), 1)
    sub = lax.broadcasted_iota(jnp.int32, (SUBS, LANES), 0)
    count = []
    which = lax.broadcasted_iota(jnp.int32, (sources, LANES), 0)
    for h in range(halves):
        block = (lane % rows) * segs + h * fold + lane // rows

        def of_block(ref):
            got = lane_gather(ref[0:1, :], block % LANES)
            for c in range(1, wide):
                got = jnp.where(block // LANES == c, lane_gather(ref[c : c + 1, :], block % LANES), got)
            return got

        count.append(of_block(count_v))
        hit = jnp.broadcast_to(of_block(source_v)[0:1, :], (sources, LANES)) == which
        one = jnp.where(hit, 1.0, 0.0).astype(jnp.bfloat16)
        for k in range(2):
            at = (k * halves + h) * LANES
            member[:, at : at + LANES] = one

    def turn(value):
        parts = [value] + [pltpu.roll(value, LANES - e * span, 1) for e in range(1, fold)]
        turned = jnp.transpose(jnp.concatenate(parts, axis=0))
        return [turned[h * fold * span : h * fold * span + span, :] for h in range(halves)]

    for h, knot in enumerate(turn(knot_v[...])):
        at = slice(h * span, h * span + span)
        low[at, :] = knot % LANES
        high[at, :] = knot // LANES

    pltpu.make_async_copy(reals, reals, real_sem).wait()
    turned = [turn(ref[...]) for ref in (phase_v, time_v, parallax_v, observed_v)]
    for h in range(halves):
        at = slice(h * span, h * span + span)
        u, time, parallax, observed = (t[h] for t in turned)
        slot = lax.broadcasted_iota(jnp.int32, (span, LANES), 0)
        live = slot < jnp.broadcast_to(count[h][0:1, :], (span, LANES))
        u2, v = u * u, 1.0 - u
        u3 = u2 * u
        spline = (
            v * v * v * (1.0 / 6.0),
            0.5 * u3 - u2 + (2.0 / 3.0),
            0.5 * (u + u2 - u3) + (1.0 / 6.0),
            u3 * (1.0 / 6.0),
        )
        for i in range(4):
            weight[i, at, :] = jnp.where(live, spline[i], 0.0)
        parallax = jnp.where(live, parallax, 0.0)
        fact[0, at, :] = time
        fact[1, at, :] = time * time
        fact[2, at, :] = parallax
        fact[3, at, :] = parallax * time
        fact[4, at, :] = observed
        both = parallax * parallax
        total = both[:SUBS]
        for g in range(1, steps):
            total = total + both[g * SUBS : (g + 1) * SUBS]
        square[h] = total

    per = table.shape[2] // LANES

    def mask_weights(chunk):
        lows, highs = low[...], high[...]
        for i in range(4):
            there = highs + (lows >= LANES - i).astype(jnp.int32) if i else highs
            masked[i] = jnp.where(there == chunk, weight[i], 0.0)

    def rows_of(source, p, first):
        at = slice(p * LANES, (p + 1) * LANES)
        here = mine[:, at] if first else table[source, :, at]
        return [here] + [pltpu.roll(here, LANES - i, 1) for i in range(1, 4)]

    def gather(shifted, v, carry):
        at = slice(v * SUBS, v * SUBS + SUBS)
        index = low[at, :]
        got = list(carry) if carry else [None] * 4
        for i in range(4):
            scale = masked[i, at, :]
            for m in range(4):
                term = lane_gather(shifted[i][m : m + 1, :], index) * scale
                got[m] = term if got[m] is None else got[m] + term
        return got

    pieces = [(sky, None, p) for p in range(per)]
    for source, here in arrivals:
        pieces += [(source, here if p == 0 else None, p) for p in range(per)]
    for n, (source, here, p) in enumerate(pieces):
        mask_weights(source * per + p)
        if n + 1 == len(pieces):
            others = table.at[: n_sky - 1]
            pltpu.make_async_copy(others, others, send_sem).wait()
        if here is not None:
            arrived = table.at[source]
            pltpu.make_async_copy(arrived, arrived, att_recv.at[here]).wait()
        shifted = rows_of(source, p, n < per)
        if n + 1 < len(pieces):
            for v in range(rows // SUBS):
                at = slice(v * SUBS, v * SUBS + SUBS)
                got = gather(shifted, v, [quat[m, at, :] for m in range(4)] if n else None)
                for m in range(4):
                    quat[m, at, :] = got[m]

    stacked = []
    for h in range(halves):
        sums = None
        for g in range(steps):
            v = h * steps + g
            at = slice(v * SUBS, v * SUBS + SUBS)
            carry = [quat[m, at, :] for m in range(4)] if len(pieces) > 1 else None
            q0, q1, q2, q3 = gather(shifted, v, carry)
            cross = (q0 * q0 + q1 * q1) - (q2 * q2 + q3 * q3)
            along = 2.0 * (q1 * q2 + q0 * q3)
            tilt = 2.0 * (q1 * q3 - q0 * q2)
            t, tt, p, tp, o = (fact[i, at, :] for i in range(5))
            rest = o - tilt
            cc, ca, aa = cross * cross, cross * along, along * along
            cr, ar = cross * rest, along * rest
            new = {
                (0, 0): cc, (0, 1): ca, (0, 3): t * cc, (0, 4): t * ca, (1, 1): aa, (1, 4): t * aa,
                (3, 3): tt * cc, (3, 4): tt * ca, (4, 4): tt * aa,
                (0, 2): p * cross, (1, 2): p * along, (2, 3): tp * cross, (2, 4): tp * along,
                0: cr, 1: ar, 2: p * rest, 3: t * cr, 4: t * ar,
            }
            sums = new if sums is None else {key: sums[key] + new[key] for key in new}
        sums[2, 2] = square[h]
        line = [sums[key] for key in sorted(sums, key=lambda key: PLACE[key])]
        groups = [fold_subs(line[i : i + SUBS], sub) for i in range(0, SUMS, SUBS)]
        groups += [jnp.zeros_like(groups[0])] * (ROWS // SUBS - len(groups))
        stacked.append(jnp.concatenate(groups, axis=0))
    for h, value in enumerate(stacked):
        for k, part in enumerate(split2(value)):
            at = (k * halves + h) * LANES
            packed[:, at : at + LANES] = part

    @pl.when(above > 0)
    def _():
        pl.semaphore_wait(met, above)

    normal = lax.dot_general(
        member[...], packed[...], (((1,), (1,)), ((), ())), preferred_element_type=jnp.float32
    )
    tiles[:, :, :ROWS] = normal.reshape(n_tm, owned, ROWS)

    for d in range(1, n_tm):
        peer = lax.rem(tm + d, n_tm)
        pltpu.make_async_remote_copy(
            src_ref=tiles.at[peer],
            dst_ref=landed.at[d - 1],
            send_sem=send_sem,
            recv_sem=sum_recv,
            device_id={"tm": peer},
            device_id_type=MESH,
        ).start()
    prior_copy.wait()
    total = tiles[tm]
    pltpu.make_async_copy(landed, landed, sum_recv).wait()
    for d in range(1, n_tm):
        total = total + landed[d - 1]
    flat[...] = jnp.transpose(total)[:ROWS]
    result = solve_rows(lambda i: flat[i : i + 1, :], lambda i: prior_ref[i : i + 1, :])
    for i in range(5):
        out_ref[i : i + 1, :] = result[i]
    pltpu.make_async_copy(landed, landed, send_sem).wait()


def on_device(n_sky, n_tm, attitude, time, parallax, observed, phase, knot, source, count, prior):
    slots, blocks, owned = time.shape[0], source.shape[0], prior.shape[1]
    knots = attitude.shape[2]
    rows = slots // LANES
    span = slots // blocks
    sources = owned * n_tm
    shape = (rows, LANES)
    vmem = pltpu.VMEM
    f32, i32, bf16 = jnp.float32, jnp.int32, jnp.bfloat16
    halves = (LANES // span) // (LANES // rows)
    return pl.pallas_call(
        functools.partial(kernel, n_sky, n_tm, span),
        out_shape=pltpu.VMEM(prior.shape, f32),
        in_specs=[pl.BlockSpec(memory_space=pl.ANY)] * 9,
        out_specs=pl.BlockSpec(memory_space=pltpu.VMEM),
        scratch_shapes=[
            vmem((4, knots), f32),
            vmem((n_sky, 4, knots), f32),
            vmem((4,) + shape, f32),
            vmem((rows + 2 * (blocks // LANES), LANES), i32),
            vmem(shape, i32),
            vmem(shape, i32),
            vmem((4,) + shape, f32),
            vmem((4,) + shape, f32),
            vmem((5,) + shape, f32),
            vmem((4,) + shape, f32),
            vmem((halves, SUBS, LANES), f32),
            vmem((sources, 2 * blocks), bf16),
            vmem((n_tm, owned, LANES), f32),
            vmem((n_tm - 1, owned, LANES), f32),
        ]
        + [pltpu.SemaphoreType.DMA] * 3
        + [pltpu.SemaphoreType.DMA((n_sky - 1,))]
        + [pltpu.SemaphoreType.DMA]
        + [pltpu.SemaphoreType.REGULAR]
        + [vmem(prior.shape, f32), vmem((ROWS, owned), f32), vmem((ROWS, 2 * blocks), bf16)],
        compiler_params=pltpu.CompilerParams(collective_id=0, has_side_effects=True),
    )(
        attitude.reshape(4, knots),
        time.reshape(shape),
        parallax.reshape(shape),
        observed.reshape(shape),
        phase.reshape(shape),
        knot.reshape(shape),
        source.reshape(blocks // LANES, LANES),
        count.reshape(blocks // LANES, LANES),
        prior,
    )


def solution(mesh):
    slot = P(("sky", "tm"))
    in_specs = (P(None, "tm", "sky"),) + (slot,) * 7 + (P(None, ("sky", "tm")),)
    return jax.shard_map(
        functools.partial(on_device, mesh.shape["sky"], mesh.shape["tm"]),
        mesh=mesh,
        in_specs=in_specs,
        out_specs=P(None, ("sky", "tm")),
        check_vma=False,
    )
```

```python
import functools

import jax
import jax.numpy as jnp
from jax import lax
from jax.experimental import pallas as pl
from jax.experimental.pallas import tpu as pltpu
from jax.sharding import PartitionSpec as P

PAIR_LIST = [(i, j) for i in range(5) for j in range(i, 5)]
MESH = pl.DeviceIdType.MESH
LANES = 128
SUBS = 8
ROWS = 32


def lane_gather(row, index):
    wide = jnp.broadcast_to(row, index.shape)
    return jnp.take_along_axis(wide, index, axis=1, mode="promise_in_bounds")


def split2(value):
    high = value.astype(jnp.bfloat16)
    return high, (value - high.astype(jnp.float32)).astype(jnp.bfloat16)


def solve_rows(row, prior_row):
    entry = {}
    for i, j in PAIR_LIST:
        entry[j, i] = row(PLACE[i, j])
    for i in range(5):
        entry[i, i] = entry[i, i] + prior_row(i)
    right = [row(PLACE[i]) for i in range(5)]
    unit, inverse = {}, []
    for col in range(5):
        inv = 1.0 / entry[col, col]
        inverse.append(inv)
        for r in range(col + 1, 5):
            unit[r, col] = entry[r, col] * inv
        for r in range(col + 1, 5):
            for c in range(col + 1, r + 1):
                entry[r, c] = entry[r, c] - unit[r, col] * entry[c, col]
            right[r] = right[r] - unit[r, col] * right[col]
    result = [right[i] * inverse[i] for i in range(5)]
    for i in range(4, 0, -1):
        for k in range(i):
            result[k] = result[k] - unit[i, k] * result[i]
    return result


PLACE = {
    (0, 0): 0, (0, 1): 1, (0, 3): 2, (0, 4): 3, (1, 3): 3, (1, 1): 4, (1, 4): 5, (3, 3): 6, (3, 4): 7,
    (4, 4): 8, (0, 2): 9, (1, 2): 10, (2, 3): 11, (2, 4): 12, 0: 13, 1: 14, 2: 15,
    3: 16, 4: 17, (2, 2): 18,
}
SUMS = 19


def orders(tm, n_tm):
    if n_tm % 2 == 0 and n_tm <= 8:

        def order(peer):
            up, across = peer // 2, peer % 2
            earlier = jnp.logical_and(tm // 2 >= up, tm % 2 >= across)
            later = jnp.logical_and(tm // 2 <= up, tm % 2 <= across)
            return jnp.logical_and(earlier, tm != peer), jnp.logical_and(later, tm != peer)
    else:

        def order(peer):
            return tm > peer, tm < peer

    return [(peer, *order(peer)) for peer in range(n_tm)]


def sky_peers(sky, n_sky):
    if n_sky & (n_sky - 1):
        sends = [(lax.rem(sky + d, n_sky), d - 1) for d in range(1, n_sky)]
        return sends, [(lax.rem(sky + n_sky - d, n_sky), d - 1) for d in range(1, n_sky)]
    core = sky % 2
    mate = sky + 1 - 2 * core
    sends, arrivals = [], [(mate, 0)]
    for k in range(1, n_sky // 2):
        base = sky - core
        for bit in [1 << i for i in range(1, n_sky.bit_length())]:
            if 2 * k & bit:
                base = base + bit * (1 - 2 * ((sky // bit) % 2))
        sends += [(base, 2 * k - 1 + core), (base + 1, 2 * k - 1 + core)]
        arrivals += [(base + 1, 2 * k), (base, 2 * k - 1)]
    return sends + [(mate, 0)], arrivals


def tell(semaphore, sky, peer, exists):
    @pl.when(exists)
    def _():
        there = {"sky": sky, "tm": peer}
        pl.semaphore_signal(semaphore, inc=1, device_id=there, device_id_type=MESH)


def fold_subs(values, sub):
    values = list(values) + [jnp.zeros_like(values[0])] * (SUBS - len(values))
    values = [values[i] for i in (0, 4, 2, 6, 1, 5, 3, 7)]
    step = 1
    while step < SUBS:
        low = (sub // step) % 2 == 0
        half = len(values) // 2
        values = [
            jnp.where(low, a, b) + pltpu.roll(jnp.where(low, b, a), step, 0)
            for a, b in zip(values[:half], values[half:])
        ]
        step *= 2
    return values[0]


def kernel(
    n_sky, n_tm, span,
    attitude_hbm, time_hbm, parallax_hbm, observed_hbm, phase_hbm, knot_hbm,
    source_hbm, count_hbm, prior_hbm,
    out_ref,
    mine, table, reals, ints, low, high, weight, masked, fact, quat, square, member, tiles, landed,
    real_sem, int_sem, send_sem, prior_sem, slot_recv, att_recv, sum_recv, met, got_reals, got_ints, prior_ref, flat, packed,
):
    own = pltpu.make_async_copy(attitude_hbm, mine, send_sem)
    own.start()
    sky = lax.axis_index("sky")
    tm = lax.axis_index("tm")
    rows = time_hbm.shape[0]
    owned = tiles.shape[1]
    wide = source_hbm.shape[0]
    phase_v, time_v, parallax_v, observed_v = (reals.at[i] for i in range(4))
    knot_v = ints.at[:rows]
    source_v = ints.at[rows : rows + wide]
    count_v = ints.at[rows + wide :]
    sources = owned * n_tm
    segs = LANES // span
    fold = LANES // rows
    halves = segs // fold
    steps = span // SUBS

    barrier = pltpu.get_barrier_semaphore()
    sends, arrivals = sky_peers(sky, n_sky)
    for peer, _ in sends:
        pl.semaphore_signal(barrier, inc=1, device_id={"sky": peer}, device_id_type=MESH)
    for src, dst in ((source_hbm, source_v), (count_hbm, count_v), (knot_hbm, knot_v)):
        pltpu.make_async_copy(src, dst, int_sem).start()
    for i, src in enumerate((phase_hbm, time_hbm, parallax_hbm, observed_hbm)):
        pltpu.make_async_copy(src, reals.at[i], real_sem).start()
    peers = orders(tm, n_tm)
    below = sum(earlier.astype(jnp.int32) for _, earlier, _ in peers)
    above = sum(later.astype(jnp.int32) for _, _, later in peers)
    mate = sky + 1 - 2 * (sky % 2)
    for peer, _, later in peers:
        tell(barrier, sky, peer, later)
        tell(barrier, mate, peer, later)

    tiles[...] = jnp.zeros_like(tiles)

    own.wait()
    pl.semaphore_wait(barrier, n_sky - 1 + 2 * below)
    for peer, there in sends:
        pltpu.make_async_remote_copy(
            src_ref=mine,
            dst_ref=table.at[sky],
            send_sem=send_sem,
            recv_sem=att_recv.at[there],
            device_id={"sky": peer},
            device_id_type=MESH,
        ).start()
    loaded = ((ints, got_ints, int_sem), (reals, got_reals, real_sem))
    for k, (here, there, semaphore) in enumerate(loaded):
        pltpu.make_async_copy(here, here, semaphore).wait()
        pltpu.make_async_remote_copy(
            src_ref=here,
            dst_ref=there,
            send_sem=semaphore,
            recv_sem=slot_recv.at[k],
            device_id={"sky": mate},
            device_id_type=MESH,
        ).start()
    prior_copy = pltpu.make_async_copy(prior_hbm, prior_ref, prior_sem)
    prior_copy.start()
    for peer, earlier, _ in peers:
        tell(met, mate, peer, earlier)

    pltpu.make_async_copy(got_ints, got_ints, slot_recv.at[0]).wait()
    lane = lax.broadcasted_iota(jnp.int32, (SUBS, LANES), 1)
    sub = lax.broadcasted_iota(jnp.int32, (SUBS, LANES), 0)
    count = []
    which = lax.broadcasted_iota(jnp.int32, (sources, LANES), 0)
    for h in range(halves):
        block = (lane % rows) * segs + h * fold + lane // rows

        def of_block(ref):
            got = lane_gather(ref[0:1, :], block % LANES)
            for c in range(1, wide):
                got = jnp.where(block // LANES == c, lane_gather(ref[c : c + 1, :], block % LANES), got)
            return got

        count.append(of_block(got_ints.at[rows + wide :]))
        hit = jnp.broadcast_to(of_block(got_ints.at[rows : rows + wide])[0:1, :], (sources, LANES)) == which
        one = jnp.where(hit, 1.0, 0.0).astype(jnp.bfloat16)
        for k in range(2):
            at = (k * halves + h) * LANES
            member[:, at : at + LANES] = one

    def turn(value):
        parts = [value] + [pltpu.roll(value, LANES - e * span, 1) for e in range(1, fold)]
        turned = jnp.transpose(jnp.concatenate(parts, axis=0))
        return [turned[h * fold * span : h * fold * span + span, :] for h in range(halves)]

    for h, knot in enumerate(turn(got_ints[:rows, :])):
        at = slice(h * span, h * span + span)
        low[at, :] = knot % LANES
        high[at, :] = knot // LANES

    pltpu.make_async_copy(got_reals, got_reals, slot_recv.at[1]).wait()
    turned = [turn(got_reals[i]) for i in range(4)]
    for h in range(halves):
        at = slice(h * span, h * span + span)
        u, time, parallax, observed = (t[h] for t in turned)
        slot = lax.broadcasted_iota(jnp.int32, (span, LANES), 0)
        live = slot < jnp.broadcast_to(count[h][0:1, :], (span, LANES))
        u2, v = u * u, 1.0 - u
        u3 = u2 * u
        spline = (
            v * v * v * (1.0 / 6.0),
            0.5 * u3 - u2 + (2.0 / 3.0),
            0.5 * (u + u2 - u3) + (1.0 / 6.0),
            u3 * (1.0 / 6.0),
        )
        for i in range(4):
            weight[i, at, :] = jnp.where(live, spline[i], 0.0)
        parallax = jnp.where(live, parallax, 0.0)
        fact[0, at, :] = time
        fact[1, at, :] = time * time
        fact[2, at, :] = parallax
        fact[3, at, :] = parallax * time
        fact[4, at, :] = observed
        both = parallax * parallax
        total = both[:SUBS]
        for g in range(1, steps):
            total = total + both[g * SUBS : (g + 1) * SUBS]
        square[h] = total

    per = table.shape[2] // LANES

    def mask_weights(chunk):
        lows, highs = low[...], high[...]
        for i in range(4):
            there = highs + (lows >= LANES - i).astype(jnp.int32) if i else highs
            masked[i] = jnp.where(there == chunk, weight[i], 0.0)

    def rows_of(source, p, first):
        at = slice(p * LANES, (p + 1) * LANES)
        here = mine[:, at] if first else table[source, :, at]
        return [here] + [pltpu.roll(here, LANES - i, 1) for i in range(1, 4)]

    def gather(shifted, v, carry):
        at = slice(v * SUBS, v * SUBS + SUBS)
        index = low[at, :]
        got = list(carry) if carry else [None] * 4
        for i in range(4):
            scale = masked[i, at, :]
            for m in range(4):
                term = lane_gather(shifted[i][m : m + 1, :], index) * scale
                got[m] = term if got[m] is None else got[m] + term
        return got

    pieces = [(sky, None, p) for p in range(per)]
    for source, here in arrivals:
        pieces += [(source, here if p == 0 else None, p) for p in range(per)]
    for n, (source, here, p) in enumerate(pieces):
        mask_weights(source * per + p)
        if n + 1 == len(pieces):
            others = table.at[: n_sky - 1]
            pltpu.make_async_copy(others, others, send_sem).wait()
            pltpu.make_async_copy(ints, ints, int_sem).wait()
            pltpu.make_async_copy(reals, reals, real_sem).wait()
        if here is not None:
            arrived = table.at[source]
            pltpu.make_async_copy(arrived, arrived, att_recv.at[here]).wait()
        shifted = rows_of(source, p, n < per)
        if n + 1 < len(pieces):
            for v in range(rows // SUBS):
                at = slice(v * SUBS, v * SUBS + SUBS)
                got = gather(shifted, v, [quat[m, at, :] for m in range(4)] if n else None)
                for m in range(4):
                    quat[m, at, :] = got[m]

    stacked = []
    for h in range(halves):
        sums = None
        for g in range(steps):
            v = h * steps + g
            at = slice(v * SUBS, v * SUBS + SUBS)
            carry = [quat[m, at, :] for m in range(4)] if len(pieces) > 1 else None
            q0, q1, q2, q3 = gather(shifted, v, carry)
            cross = (q0 * q0 + q1 * q1) - (q2 * q2 + q3 * q3)
            along = 2.0 * (q1 * q2 + q0 * q3)
            tilt = 2.0 * (q1 * q3 - q0 * q2)
            t, tt, p, tp, o = (fact[i, at, :] for i in range(5))
            rest = o - tilt
            cc, ca, aa = cross * cross, cross * along, along * along
            cr, ar = cross * rest, along * rest
            new = {
                (0, 0): cc, (0, 1): ca, (0, 3): t * cc, (0, 4): t * ca, (1, 1): aa, (1, 4): t * aa,
                (3, 3): tt * cc, (3, 4): tt * ca, (4, 4): tt * aa,
                (0, 2): p * cross, (1, 2): p * along, (2, 3): tp * cross, (2, 4): tp * along,
                0: cr, 1: ar, 2: p * rest, 3: t * cr, 4: t * ar,
            }
            sums = new if sums is None else {key: sums[key] + new[key] for key in new}
        sums[2, 2] = square[h]
        line = [sums[key] for key in sorted(sums, key=lambda key: PLACE[key])]
        groups = [fold_subs(line[i : i + SUBS], sub) for i in range(0, SUMS, SUBS)]
        groups += [jnp.zeros_like(groups[0])] * (ROWS // SUBS - len(groups))
        stacked.append(jnp.concatenate(groups, axis=0))
    for h, value in enumerate(stacked):
        for k, part in enumerate(split2(value)):
            at = (k * halves + h) * LANES
            packed[:, at : at + LANES] = part

    @pl.when(above > 0)
    def _():
        pl.semaphore_wait(met, above)

    normal = lax.dot_general(
        member[...], packed[...], (((1,), (1,)), ((), ())), preferred_element_type=jnp.float32
    )
    tiles[:, :, :ROWS] = normal.reshape(n_tm, owned, ROWS)

    for d in (*range(1, n_tm), 0):
        peer = lax.rem(tm + d, n_tm)
        pltpu.make_async_remote_copy(
            src_ref=tiles.at[peer],
            dst_ref=landed.at[d],
            send_sem=send_sem,
            recv_sem=sum_recv,
            device_id={"sky": mate, "tm": peer},
            device_id_type=MESH,
        ).start()
    prior_copy.wait()
    pltpu.make_async_copy(landed, landed, sum_recv).wait()
    total = landed[0]
    for d in range(1, n_tm):
        total = total + landed[d]
    flat[...] = jnp.transpose(total)[:ROWS]
    result = solve_rows(lambda i: flat[i : i + 1, :], lambda i: prior_ref[i : i + 1, :])
    for i in range(5):
        out_ref[i : i + 1, :] = result[i]
    pltpu.make_async_copy(landed, landed, send_sem).wait()


def on_device(n_sky, n_tm, attitude, time, parallax, observed, phase, knot, source, count, prior):
    slots, blocks, owned = time.shape[0], source.shape[0], prior.shape[1]
    knots = attitude.shape[2]
    rows = slots // LANES
    span = slots // blocks
    sources = owned * n_tm
    shape = (rows, LANES)
    vmem = pltpu.VMEM
    f32, i32, bf16 = jnp.float32, jnp.int32, jnp.bfloat16
    halves = (LANES // span) // (LANES // rows)
    return pl.pallas_call(
        functools.partial(kernel, n_sky, n_tm, span),
        out_shape=pltpu.VMEM(prior.shape, f32),
        in_specs=[pl.BlockSpec(memory_space=pl.ANY)] * 9,
        out_specs=pl.BlockSpec(memory_space=pltpu.VMEM),
        scratch_shapes=[
            vmem((4, knots), f32),
            vmem((n_sky, 4, knots), f32),
            vmem((4,) + shape, f32),
            vmem((rows + 2 * (blocks // LANES), LANES), i32),
            vmem(shape, i32),
            vmem(shape, i32),
            vmem((4,) + shape, f32),
            vmem((4,) + shape, f32),
            vmem((5,) + shape, f32),
            vmem((4,) + shape, f32),
            vmem((halves, SUBS, LANES), f32),
            vmem((sources, 2 * blocks), bf16),
            vmem((n_tm, owned, LANES), f32),
            vmem((n_tm, owned, LANES), f32),
        ]
        + [pltpu.SemaphoreType.DMA] * 4
        + [pltpu.SemaphoreType.DMA((2,))]
        + [pltpu.SemaphoreType.DMA((n_sky - 1,))]
        + [pltpu.SemaphoreType.DMA]
        + [pltpu.SemaphoreType.REGULAR]
        + [vmem((4,) + shape, f32), vmem((rows + 2 * (blocks // LANES), LANES), i32)]
        + [vmem(prior.shape, f32), vmem((ROWS, owned), f32), vmem((ROWS, 2 * blocks), bf16)],
        compiler_params=pltpu.CompilerParams(collective_id=0, has_side_effects=True),
    )(
        attitude.reshape(4, knots),
        time.reshape(shape),
        parallax.reshape(shape),
        observed.reshape(shape),
        phase.reshape(shape),
        knot.reshape(shape),
        source.reshape(blocks // LANES, LANES),
        count.reshape(blocks // LANES, LANES),
        prior,
    )


def solution(mesh):
    slot = P(("sky", "tm"))
    in_specs = (P(None, "tm", "sky"),) + (slot,) * 7 + (P(None, ("sky", "tm")),)
    return jax.shard_map(
        functools.partial(on_device, mesh.shape["sky"], mesh.shape["tm"]),
        mesh=mesh,
        in_specs=in_specs,
        out_specs=P(None, ("sky", "tm")),
        check_vma=False,
    )
```

```python
import functools

import jax
import jax.numpy as jnp
from jax import lax
from jax.experimental import pallas as pl
from jax.experimental.pallas import tpu as pltpu
from jax.sharding import PartitionSpec as P

PAIR_LIST = [(i, j) for i in range(5) for j in range(i, 5)]
MESH = pl.DeviceIdType.MESH
LANES = 128
SUBS = 8
ROWS = 32


def lane_gather(row, index):
    wide = jnp.broadcast_to(row, index.shape)
    return jnp.take_along_axis(wide, index, axis=1, mode="promise_in_bounds")


def split2(value):
    high = value.astype(jnp.bfloat16)
    return high, (value - high.astype(jnp.float32)).astype(jnp.bfloat16)


def solve_rows(row, prior_row):
    entry = {}
    for i, j in PAIR_LIST:
        entry[j, i] = row(PLACE[i, j])
    for i in range(5):
        entry[i, i] = entry[i, i] + prior_row(i)
    right = [row(PLACE[i]) for i in range(5)]
    unit, inverse = {}, []
    for col in range(5):
        inv = 1.0 / entry[col, col]
        inverse.append(inv)
        for r in range(col + 1, 5):
            unit[r, col] = entry[r, col] * inv
        for r in range(col + 1, 5):
            for c in range(col + 1, r + 1):
                entry[r, c] = entry[r, c] - unit[r, col] * entry[c, col]
            right[r] = right[r] - unit[r, col] * right[col]
    result = [right[i] * inverse[i] for i in range(5)]
    for i in range(4, 0, -1):
        for k in range(i):
            result[k] = result[k] - unit[i, k] * result[i]
    return result


PLACE = {
    (0, 0): 0, (0, 1): 1, (0, 3): 2, (0, 4): 3, (1, 3): 3, (1, 1): 4, (1, 4): 5, (3, 3): 6, (3, 4): 7,
    (4, 4): 8, (0, 2): 9, (1, 2): 10, (2, 3): 11, (2, 4): 12, 0: 13, 1: 14, 2: 15,
    3: 16, 4: 17, (2, 2): 18,
}
SUMS = 19


def orders(tm, n_tm):
    if n_tm % 2 == 0 and n_tm <= 8:

        def order(peer):
            up, across = peer // 2, peer % 2
            earlier = jnp.logical_and(tm // 2 >= up, tm % 2 >= across)
            later = jnp.logical_and(tm // 2 <= up, tm % 2 <= across)
            return jnp.logical_and(earlier, tm != peer), jnp.logical_and(later, tm != peer)
    else:

        def order(peer):
            return tm > peer, tm < peer

    return [(peer, *order(peer)) for peer in range(n_tm)]


def sky_peers(sky, n_sky):
    if n_sky & (n_sky - 1):
        sends = [(lax.rem(sky + d, n_sky), d - 1) for d in range(1, n_sky)]
        return sends, [(lax.rem(sky + n_sky - d, n_sky), d - 1) for d in range(1, n_sky)]
    core = sky % 2
    mate = sky + 1 - 2 * core
    sends, arrivals = [], [(mate, 0)]
    for k in range(1, n_sky // 2):
        base = sky - core
        for bit in [1 << i for i in range(1, n_sky.bit_length())]:
            if 2 * k & bit:
                base = base + bit * (1 - 2 * ((sky // bit) % 2))
        sends += [(base, 2 * k - 1 + core), (base + 1, 2 * k - 1 + core)]
        arrivals += [(base + 1, 2 * k), (base, 2 * k - 1)]
    return sends + [(mate, 0)], arrivals


def tell(semaphore, sky, peer, exists):
    @pl.when(exists)
    def _():
        there = {"sky": sky, "tm": peer}
        pl.semaphore_signal(semaphore, inc=1, device_id=there, device_id_type=MESH)


def fold_subs(values, sub):
    values = list(values) + [jnp.zeros_like(values[0])] * (SUBS - len(values))
    values = [values[i] for i in (0, 4, 2, 6, 1, 5, 3, 7)]
    step = 1
    while step < SUBS:
        low = (sub // step) % 2 == 0
        half = len(values) // 2
        values = [
            jnp.where(low, a, b) + pltpu.roll(jnp.where(low, b, a), step, 0)
            for a, b in zip(values[:half], values[half:])
        ]
        step *= 2
    return values[0]


def kernel(
    n_sky, n_tm, span,
    attitude_hbm, time_hbm, parallax_hbm, observed_hbm, phase_hbm, knot_hbm,
    source_hbm, count_hbm, prior_hbm,
    out_ref,
    mine, table, reals, ints, low, high, weight, masked, fact, quat, square, member, tiles, landed,
    real_sem, int_sem, send_sem, prior_sem, slot_recv, att_recv, sum_recv, met, got_reals, got_ints, prior_ref, flat, packed,
):
    own = pltpu.make_async_copy(attitude_hbm, mine, send_sem)
    own.start()
    sky = lax.axis_index("sky")
    tm = lax.axis_index("tm")
    rows = time_hbm.shape[0]
    owned = tiles.shape[1]
    wide = source_hbm.shape[0]
    phase_v, time_v, parallax_v, observed_v = (reals.at[i] for i in range(4))
    knot_v = ints.at[:rows]
    source_v = ints.at[rows : rows + wide]
    count_v = ints.at[rows + wide :]
    sources = owned * n_tm
    segs = LANES // span
    fold = LANES // rows
    halves = segs // fold
    steps = span // SUBS

    barrier = pltpu.get_barrier_semaphore()
    sends, arrivals = sky_peers(sky, n_sky)
    for peer, _ in sends:
        pl.semaphore_signal(barrier, inc=1, device_id={"sky": peer}, device_id_type=MESH)
    for src, dst in ((source_hbm, source_v), (count_hbm, count_v), (knot_hbm, knot_v)):
        pltpu.make_async_copy(src, dst, int_sem).start()
    for i, src in enumerate((phase_hbm, time_hbm, parallax_hbm, observed_hbm)):
        pltpu.make_async_copy(src, reals.at[i], real_sem).start()
    peers = orders(tm, n_tm)
    below = sum(earlier.astype(jnp.int32) for _, earlier, _ in peers)
    above = sum(later.astype(jnp.int32) for _, _, later in peers)
    mate = sky + 1 - 2 * (sky % 2)
    for peer, _, later in peers:
        tell(barrier, sky, peer, later)
        tell(barrier, mate, peer, later)

    tiles[...] = jnp.zeros_like(tiles)

    own.wait()
    pl.semaphore_wait(barrier, n_sky - 1 + 2 * below)
    for peer, there in sends:
        pltpu.make_async_remote_copy(
            src_ref=mine,
            dst_ref=table.at[sky],
            send_sem=send_sem,
            recv_sem=att_recv.at[there],
            device_id={"sky": peer},
            device_id_type=MESH,
        ).start()
    loaded = ((ints, got_ints, int_sem), (reals, got_reals, real_sem))
    for k, (here, there, semaphore) in enumerate(loaded):
        pltpu.make_async_copy(here, here, semaphore).wait()
        pltpu.make_async_remote_copy(
            src_ref=here,
            dst_ref=there,
            send_sem=semaphore,
            recv_sem=slot_recv.at[k],
            device_id={"sky": mate},
            device_id_type=MESH,
        ).start()
    prior_copy = pltpu.make_async_copy(prior_hbm, prior_ref, prior_sem)
    prior_copy.start()
    for peer, earlier, _ in peers:
        tell(met, mate, peer, earlier)

    pltpu.make_async_copy(got_ints, got_ints, slot_recv.at[0]).wait()
    lane = lax.broadcasted_iota(jnp.int32, (SUBS, LANES), 1)
    sub = lax.broadcasted_iota(jnp.int32, (SUBS, LANES), 0)
    count = []
    which = lax.broadcasted_iota(jnp.int32, (sources, LANES), 0)
    for h in range(halves):
        block = (lane % rows) * segs + h * fold + lane // rows

        def of_block(ref):
            got = lane_gather(ref[0:1, :], block % LANES)
            for c in range(1, wide):
                got = jnp.where(block // LANES == c, lane_gather(ref[c : c + 1, :], block % LANES), got)
            return got

        count.append(of_block(got_ints.at[rows + wide :]))
        hit = jnp.broadcast_to(of_block(got_ints.at[rows : rows + wide])[0:1, :], (sources, LANES)) == which
        one = jnp.where(hit, 1.0, 0.0).astype(jnp.bfloat16)
        for k in range(2):
            at = (k * halves + h) * LANES
            member[:, at : at + LANES] = one

    def turn(value):
        parts = [value] + [pltpu.roll(value, LANES - e * span, 1) for e in range(1, fold)]
        turned = jnp.transpose(jnp.concatenate(parts, axis=0))
        return [turned[h * fold * span : h * fold * span + span, :] for h in range(halves)]

    for h, knot in enumerate(turn(got_ints[:rows, :])):
        at = slice(h * span, h * span + span)
        low[at, :] = knot % LANES
        high[at, :] = knot // LANES

    pltpu.make_async_copy(got_reals, got_reals, slot_recv.at[1]).wait()
    turned = [turn(got_reals[i]) for i in range(4)]
    for h in range(halves):
        at = slice(h * span, h * span + span)
        u, time, parallax, observed = (t[h] for t in turned)
        slot = lax.broadcasted_iota(jnp.int32, (span, LANES), 0)
        live = slot < jnp.broadcast_to(count[h][0:1, :], (span, LANES))
        u2, v = u * u, 1.0 - u
        u3 = u2 * u
        spline = (
            v * v * v * (1.0 / 6.0),
            0.5 * u3 - u2 + (2.0 / 3.0),
            0.5 * (u + u2 - u3) + (1.0 / 6.0),
            u3 * (1.0 / 6.0),
        )
        for i in range(4):
            weight[i, at, :] = jnp.where(live, spline[i], 0.0)
        parallax = jnp.where(live, parallax, 0.0)
        fact[0, at, :] = time
        fact[1, at, :] = time * time
        fact[2, at, :] = parallax
        fact[3, at, :] = parallax * time
        fact[4, at, :] = observed
        both = parallax * parallax
        total = both[:SUBS]
        for g in range(1, steps):
            total = total + both[g * SUBS : (g + 1) * SUBS]
        square[h] = total

    per = table.shape[2] // LANES

    def mask_weights(slot, chunk):
        lows, highs = low[...], high[...]
        for i in range(4):
            there = highs + (lows >= LANES - i).astype(jnp.int32) if i else highs
            masked[slot, i] = jnp.where(there == chunk, weight[i], 0.0)

    def rows_of(source, p, first):
        at = slice(p * LANES, (p + 1) * LANES)
        here = mine[:, at] if first else table[source, :, at]
        return [here] + [pltpu.roll(here, LANES - i, 1) for i in range(1, 4)]

    def gather(group, v, carry):
        at = slice(v * SUBS, v * SUBS + SUBS)
        index = low[at, :]
        got = list(carry) if carry else [None] * 4
        for slot, shifted in enumerate(group):
            for i in range(4):
                scale = masked[slot, i, at, :]
                for m in range(4):
                    term = lane_gather(shifted[i][m : m + 1, :], index) * scale
                    got[m] = term if got[m] is None else got[m] + term
        return got

    pieces = [(sky, None, p, True) for p in range(per)]
    for source, here in arrivals:
        pieces += [(source, here if p == 0 else None, p, False) for p in range(per)]
    ahead = 2 if len(pieces) > 2 else 1
    groups = [pieces[:ahead]] + [[piece] for piece in pieces[ahead:]]
    for n, group in enumerate(groups):
        for slot, (source, here, p, first) in enumerate(group):
            mask_weights(slot, source * per + p)
        if n + 1 == len(groups):
            others = table.at[: n_sky - 1]
            pltpu.make_async_copy(others, others, send_sem).wait()
            pltpu.make_async_copy(ints, ints, int_sem).wait()
            pltpu.make_async_copy(reals, reals, real_sem).wait()
        for source, here, p, first in group:
            if here is not None:
                arrived = table.at[source]
                pltpu.make_async_copy(arrived, arrived, att_recv.at[here]).wait()
        shifted = [rows_of(source, p, first) for source, here, p, first in group]
        if n + 1 < len(groups):
            for v in range(rows // SUBS):
                at = slice(v * SUBS, v * SUBS + SUBS)
                got = gather(shifted, v, [quat[m, at, :] for m in range(4)] if n else None)
                for m in range(4):
                    quat[m, at, :] = got[m]

    stacked = []
    for h in range(halves):
        sums = None
        for g in range(steps):
            v = h * steps + g
            at = slice(v * SUBS, v * SUBS + SUBS)
            carry = [quat[m, at, :] for m in range(4)] if len(groups) > 1 else None
            q0, q1, q2, q3 = gather(shifted, v, carry)
            cross = (q0 * q0 + q1 * q1) - (q2 * q2 + q3 * q3)
            along = 2.0 * (q1 * q2 + q0 * q3)
            tilt = 2.0 * (q1 * q3 - q0 * q2)
            t, tt, p, tp, o = (fact[i, at, :] for i in range(5))
            rest = o - tilt
            cc, ca, aa = cross * cross, cross * along, along * along
            cr, ar = cross * rest, along * rest
            new = {
                (0, 0): cc, (0, 1): ca, (0, 3): t * cc, (0, 4): t * ca, (1, 1): aa, (1, 4): t * aa,
                (3, 3): tt * cc, (3, 4): tt * ca, (4, 4): tt * aa,
                (0, 2): p * cross, (1, 2): p * along, (2, 3): tp * cross, (2, 4): tp * along,
                0: cr, 1: ar, 2: p * rest, 3: t * cr, 4: t * ar,
            }
            sums = new if sums is None else {key: sums[key] + new[key] for key in new}
        sums[2, 2] = square[h]
        line = [sums[key] for key in sorted(sums, key=lambda key: PLACE[key])]
        groups = [fold_subs(line[i : i + SUBS], sub) for i in range(0, SUMS, SUBS)]
        groups += [jnp.zeros_like(groups[0])] * (ROWS // SUBS - len(groups))
        stacked.append(jnp.concatenate(groups, axis=0))
    for h, value in enumerate(stacked):
        for k, part in enumerate(split2(value)):
            at = (k * halves + h) * LANES
            packed[:, at : at + LANES] = part

    @pl.when(above > 0)
    def _():
        pl.semaphore_wait(met, above)

    normal = lax.dot_general(
        member[...], packed[...], (((1,), (1,)), ((), ())), preferred_element_type=jnp.float32
    )
    tiles[:, :, :ROWS] = normal.reshape(n_tm, owned, ROWS)

    for d in (*range(1, n_tm), 0):
        peer = lax.rem(tm + d, n_tm)
        pltpu.make_async_remote_copy(
            src_ref=tiles.at[peer],
            dst_ref=landed.at[d],
            send_sem=send_sem,
            recv_sem=sum_recv,
            device_id={"sky": mate, "tm": peer},
            device_id_type=MESH,
        ).start()
    prior_copy.wait()
    pltpu.make_async_copy(landed, landed, sum_recv).wait()
    total = landed[0]
    for d in range(1, n_tm):
        total = total + landed[d]
    flat[...] = jnp.transpose(total)[:ROWS]
    result = solve_rows(lambda i: flat[i : i + 1, :], lambda i: prior_ref[i : i + 1, :])
    for i in range(5):
        out_ref[i : i + 1, :] = result[i]
    pltpu.make_async_copy(landed, landed, send_sem).wait()


def on_device(n_sky, n_tm, attitude, time, parallax, observed, phase, knot, source, count, prior):
    slots, blocks, owned = time.shape[0], source.shape[0], prior.shape[1]
    knots = attitude.shape[2]
    rows = slots // LANES
    span = slots // blocks
    sources = owned * n_tm
    shape = (rows, LANES)
    vmem = pltpu.VMEM
    f32, i32, bf16 = jnp.float32, jnp.int32, jnp.bfloat16
    halves = (LANES // span) // (LANES // rows)
    return pl.pallas_call(
        functools.partial(kernel, n_sky, n_tm, span),
        out_shape=pltpu.VMEM(prior.shape, f32),
        in_specs=[pl.BlockSpec(memory_space=pl.ANY)] * 9,
        out_specs=pl.BlockSpec(memory_space=pltpu.VMEM),
        scratch_shapes=[
            vmem((4, knots), f32),
            vmem((n_sky, 4, knots), f32),
            vmem((4,) + shape, f32),
            vmem((rows + 2 * (blocks // LANES), LANES), i32),
            vmem(shape, i32),
            vmem(shape, i32),
            vmem((4,) + shape, f32),
            vmem((2, 4) + shape, f32),
            vmem((5,) + shape, f32),
            vmem((4,) + shape, f32),
            vmem((halves, SUBS, LANES), f32),
            vmem((sources, 2 * blocks), bf16),
            vmem((n_tm, owned, LANES), f32),
            vmem((n_tm, owned, LANES), f32),
        ]
        + [pltpu.SemaphoreType.DMA] * 4
        + [pltpu.SemaphoreType.DMA((2,))]
        + [pltpu.SemaphoreType.DMA((n_sky - 1,))]
        + [pltpu.SemaphoreType.DMA]
        + [pltpu.SemaphoreType.REGULAR]
        + [vmem((4,) + shape, f32), vmem((rows + 2 * (blocks // LANES), LANES), i32)]
        + [vmem(prior.shape, f32), vmem((ROWS, owned), f32), vmem((ROWS, 2 * blocks), bf16)],
        compiler_params=pltpu.CompilerParams(collective_id=0, has_side_effects=True),
    )(
        attitude.reshape(4, knots),
        time.reshape(shape),
        parallax.reshape(shape),
        observed.reshape(shape),
        phase.reshape(shape),
        knot.reshape(shape),
        source.reshape(blocks // LANES, LANES),
        count.reshape(blocks // LANES, LANES),
        prior,
    )


def solution(mesh):
    slot = P(("sky", "tm"))
    in_specs = (P(None, "tm", "sky"),) + (slot,) * 7 + (P(None, ("sky", "tm")),)
    return jax.shard_map(
        functools.partial(on_device, mesh.shape["sky"], mesh.shape["tm"]),
        mesh=mesh,
        in_specs=in_specs,
        out_specs=P(None, ("sky", "tm")),
        check_vma=False,
    )
```

```python
import functools

import jax
import jax.numpy as jnp
from jax import lax
from jax.experimental import pallas as pl
from jax.experimental.pallas import tpu as pltpu
from jax.sharding import PartitionSpec as P

PAIR_LIST = [(i, j) for i in range(5) for j in range(i, 5)]
MESH = pl.DeviceIdType.MESH
LANES = 128
SUBS = 8
ROWS = 32


def lane_gather(row, index):
    wide = jnp.broadcast_to(row, index.shape)
    return jnp.take_along_axis(wide, index, axis=1, mode="promise_in_bounds")


def split2(value):
    high = value.astype(jnp.bfloat16)
    return high, (value - high.astype(jnp.float32)).astype(jnp.bfloat16)


def solve_rows(row, prior_row):
    entry = {}
    for i, j in PAIR_LIST:
        entry[j, i] = row(PLACE[i, j])
    for i in range(5):
        entry[i, i] = entry[i, i] + prior_row(i)
    right = [row(PLACE[i]) for i in range(5)]
    unit, inverse = {}, []
    for col in range(5):
        inv = 1.0 / entry[col, col]
        inverse.append(inv)
        for r in range(col + 1, 5):
            unit[r, col] = entry[r, col] * inv
        for r in range(col + 1, 5):
            for c in range(col + 1, r + 1):
                entry[r, c] = entry[r, c] - unit[r, col] * entry[c, col]
            right[r] = right[r] - unit[r, col] * right[col]
    result = [right[i] * inverse[i] for i in range(5)]
    for i in range(4, 0, -1):
        for k in range(i):
            result[k] = result[k] - unit[i, k] * result[i]
    return result


PLACE = {
    (0, 0): 0, (0, 1): 1, (0, 3): 2, (0, 4): 3, (1, 3): 3, (1, 1): 4, (1, 4): 5, (3, 3): 6, (3, 4): 7,
    (4, 4): 8, (0, 2): 9, (1, 2): 10, (2, 3): 11, (2, 4): 12, 0: 13, 1: 14, 2: 15,
    3: 16, 4: 17, (2, 2): 18,
}
SUMS = 19


def orders(tm, n_tm):
    if n_tm % 2 == 0 and n_tm <= 8:

        def order(peer):
            up, across = peer // 2, peer % 2
            earlier = jnp.logical_and(tm // 2 >= up, tm % 2 >= across)
            later = jnp.logical_and(tm // 2 <= up, tm % 2 <= across)
            return jnp.logical_and(earlier, tm != peer), jnp.logical_and(later, tm != peer)
    else:

        def order(peer):
            return tm > peer, tm < peer

    return [(peer, *order(peer)) for peer in range(n_tm)]


def sky_peers(sky, n_sky):
    if n_sky & (n_sky - 1):
        sends = [(lax.rem(sky + d, n_sky), d - 1) for d in range(1, n_sky)]
        return sends, [(lax.rem(sky + n_sky - d, n_sky), d - 1) for d in range(1, n_sky)]
    core = sky % 2
    mate = sky + 1 - 2 * core
    sends, arrivals = [], [(mate, 0)]
    for k in range(1, n_sky // 2):
        base = sky - core
        for bit in [1 << i for i in range(1, n_sky.bit_length())]:
            if 2 * k & bit:
                base = base + bit * (1 - 2 * ((sky // bit) % 2))
        sends += [(base, 2 * k - 1 + core), (base + 1, 2 * k - 1 + core)]
        arrivals += [(base + 1, 2 * k), (base, 2 * k - 1)]
    return sends + [(mate, 0)], arrivals


def tell(semaphore, sky, peer, exists):
    @pl.when(exists)
    def _():
        there = {"sky": sky, "tm": peer}
        pl.semaphore_signal(semaphore, inc=1, device_id=there, device_id_type=MESH)


def fold_subs(values, sub):
    values = list(values) + [jnp.zeros_like(values[0])] * (SUBS - len(values))
    values = [values[i] for i in (0, 4, 2, 6, 1, 5, 3, 7)]
    step = 1
    while step < SUBS:
        low = (sub // step) % 2 == 0
        half = len(values) // 2
        values = [
            jnp.where(low, a, b) + pltpu.roll(jnp.where(low, b, a), step, 0)
            for a, b in zip(values[:half], values[half:])
        ]
        step *= 2
    return values[0]


def kernel(
    n_sky, n_tm, span,
    attitude_hbm, time_hbm, parallax_hbm, observed_hbm, phase_hbm, knot_hbm,
    source_hbm, count_hbm, prior_hbm,
    out_ref,
    mine, table, reals, ints, low, high, weight, masked, fact, quat, square, member, tiles, landed,
    real_sem, int_sem, send_sem, slot_recv, att_recv, sum_recv, met, got_reals, got_ints, prior_ref, flat, packed,
):
    own = pltpu.make_async_copy(attitude_hbm, mine, send_sem)
    own.start()
    sky = lax.axis_index("sky")
    tm = lax.axis_index("tm")
    rows = time_hbm.shape[0]
    owned = tiles.shape[1]
    wide = source_hbm.shape[0]
    phase_v, time_v, parallax_v, observed_v = (reals.at[i] for i in range(4))
    knot_v = ints.at[:rows]
    source_v = ints.at[rows : rows + wide]
    count_v = ints.at[rows + wide :]
    sources = owned * n_tm
    segs = LANES // span
    fold = LANES // rows
    halves = segs // fold
    steps = span // SUBS

    barrier = pltpu.get_barrier_semaphore()
    sends, arrivals = sky_peers(sky, n_sky)
    for peer, _ in sends:
        pl.semaphore_signal(barrier, inc=1, device_id={"sky": peer}, device_id_type=MESH)
    for src, dst in ((source_hbm, source_v), (count_hbm, count_v), (knot_hbm, knot_v)):
        pltpu.make_async_copy(src, dst, int_sem).start()
    for i, src in enumerate((phase_hbm, time_hbm, parallax_hbm, observed_hbm)):
        pltpu.make_async_copy(src, reals.at[i], real_sem).start()
    peers = orders(tm, n_tm)
    below = sum(earlier.astype(jnp.int32) for _, earlier, _ in peers)
    above = sum(later.astype(jnp.int32) for _, _, later in peers)
    mate = sky + 1 - 2 * (sky % 2)
    for peer, _, later in peers:
        tell(barrier, sky, peer, later)
        tell(barrier, mate, peer, later)

    tiles[...] = jnp.zeros_like(tiles)

    own.wait()
    pl.semaphore_wait(barrier, n_sky - 1 + 2 * below)
    for peer, there in sends:
        pltpu.make_async_remote_copy(
            src_ref=mine,
            dst_ref=table.at[sky],
            send_sem=send_sem,
            recv_sem=att_recv.at[there],
            device_id={"sky": peer},
            device_id_type=MESH,
        ).start()
    loaded = ((ints, got_ints, int_sem), (reals, got_reals, real_sem))
    for k, (here, there, semaphore) in enumerate(loaded):
        pltpu.make_async_copy(here, here, semaphore).wait()
        pltpu.make_async_remote_copy(
            src_ref=here,
            dst_ref=there,
            send_sem=semaphore,
            recv_sem=slot_recv.at[k],
            device_id={"sky": mate},
            device_id_type=MESH,
        ).start()
    for peer, earlier, _ in peers:
        tell(met, mate, peer, earlier)

    pltpu.make_async_copy(got_ints, got_ints, slot_recv.at[0]).wait()
    lane = lax.broadcasted_iota(jnp.int32, (SUBS, LANES), 1)
    sub = lax.broadcasted_iota(jnp.int32, (SUBS, LANES), 0)
    count = []
    which = lax.broadcasted_iota(jnp.int32, (sources, LANES), 0)
    for h in range(halves):
        block = (lane % rows) * segs + h * fold + lane // rows

        def of_block(ref):
            got = lane_gather(ref[0:1, :], block % LANES)
            for c in range(1, wide):
                got = jnp.where(block // LANES == c, lane_gather(ref[c : c + 1, :], block % LANES), got)
            return got

        count.append(of_block(got_ints.at[rows + wide :]))
        hit = jnp.broadcast_to(of_block(got_ints.at[rows : rows + wide])[0:1, :], (sources, LANES)) == which
        one = jnp.where(hit, 1.0, 0.0).astype(jnp.bfloat16)
        for k in range(2):
            at = (k * halves + h) * LANES
            member[:, at : at + LANES] = one

    def turn(value):
        parts = [value] + [pltpu.roll(value, LANES - e * span, 1) for e in range(1, fold)]
        turned = jnp.transpose(jnp.concatenate(parts, axis=0))
        return [turned[h * fold * span : h * fold * span + span, :] for h in range(halves)]

    for h, knot in enumerate(turn(got_ints[:rows, :])):
        at = slice(h * span, h * span + span)
        low[at, :] = knot % LANES
        high[at, :] = knot // LANES

    pltpu.make_async_copy(got_reals, got_reals, slot_recv.at[1]).wait()
    turned = [turn(got_reals[i]) for i in range(4)]
    for h in range(halves):
        at = slice(h * span, h * span + span)
        u, time, parallax, observed = (t[h] for t in turned)
        slot = lax.broadcasted_iota(jnp.int32, (span, LANES), 0)
        live = slot < jnp.broadcast_to(count[h][0:1, :], (span, LANES))
        u2, v = u * u, 1.0 - u
        u3 = u2 * u
        spline = (
            v * v * v * (1.0 / 6.0),
            0.5 * u3 - u2 + (2.0 / 3.0),
            0.5 * (u + u2 - u3) + (1.0 / 6.0),
            u3 * (1.0 / 6.0),
        )
        for i in range(4):
            weight[i, at, :] = jnp.where(live, spline[i], 0.0)
        parallax = jnp.where(live, parallax, 0.0)
        fact[0, at, :] = time
        fact[1, at, :] = time * time
        fact[2, at, :] = parallax
        fact[3, at, :] = parallax * time
        fact[4, at, :] = observed
        both = parallax * parallax
        total = both[:SUBS]
        for g in range(1, steps):
            total = total + both[g * SUBS : (g + 1) * SUBS]
        square[h] = total

    per = table.shape[2] // LANES

    def mask_weights(slot, chunk):
        lows, highs = low[...], high[...]
        for i in range(4):
            there = highs + (lows >= LANES - i).astype(jnp.int32) if i else highs
            masked[slot, i] = jnp.where(there == chunk, weight[i], 0.0)

    def rows_of(source, p, first):
        at = slice(p * LANES, (p + 1) * LANES)
        here = mine[:, at] if first else table[source, :, at]
        return [here] + [pltpu.roll(here, LANES - i, 1) for i in range(1, 4)]

    def gather(group, v, carry):
        at = slice(v * SUBS, v * SUBS + SUBS)
        index = low[at, :]
        got = list(carry) if carry else [None] * 4
        for slot, shifted in enumerate(group):
            for i in range(4):
                scale = masked[slot, i, at, :]
                for m in range(4):
                    term = lane_gather(shifted[i][m : m + 1, :], index) * scale
                    got[m] = term if got[m] is None else got[m] + term
        return got

    pieces = [(sky, None, p, True) for p in range(per)]
    for source, here in arrivals:
        pieces += [(source, here if p == 0 else None, p, False) for p in range(per)]
    ahead = 2 if len(pieces) > 2 else 1
    groups = [pieces[:ahead]] + [[piece] for piece in pieces[ahead:]]
    for n, group in enumerate(groups):
        for slot, (source, here, p, first) in enumerate(group):
            mask_weights(slot, source * per + p)
        if n + 1 == len(groups):
            others = table.at[: n_sky - 1]
            pltpu.make_async_copy(others, others, send_sem).wait()
            pltpu.make_async_copy(ints, ints, int_sem).wait()
            pltpu.make_async_copy(reals, reals, real_sem).wait()
            prior_copy = pltpu.make_async_copy(prior_hbm, prior_ref, int_sem)
            prior_copy.start()
        for source, here, p, first in group:
            if here is not None:
                arrived = table.at[source]
                pltpu.make_async_copy(arrived, arrived, att_recv.at[here]).wait()
        shifted = [rows_of(source, p, first) for source, here, p, first in group]
        if n + 1 < len(groups):
            for v in range(rows // SUBS):
                at = slice(v * SUBS, v * SUBS + SUBS)
                got = gather(shifted, v, [quat[m, at, :] for m in range(4)] if n else None)
                for m in range(4):
                    quat[m, at, :] = got[m]

    stacked = []
    for h in range(halves):
        sums = None
        for g in range(steps):
            v = h * steps + g
            at = slice(v * SUBS, v * SUBS + SUBS)
            carry = [quat[m, at, :] for m in range(4)] if len(groups) > 1 else None
            q0, q1, q2, q3 = gather(shifted, v, carry)
            cross = (q0 * q0 + q1 * q1) - (q2 * q2 + q3 * q3)
            along = 2.0 * (q1 * q2 + q0 * q3)
            tilt = 2.0 * (q1 * q3 - q0 * q2)
            t, tt, p, tp, o = (fact[i, at, :] for i in range(5))
            rest = o - tilt
            cc, ca, aa = cross * cross, cross * along, along * along
            cr, ar = cross * rest, along * rest
            new = {
                (0, 0): cc, (0, 1): ca, (0, 3): t * cc, (0, 4): t * ca, (1, 1): aa, (1, 4): t * aa,
                (3, 3): tt * cc, (3, 4): tt * ca, (4, 4): tt * aa,
                (0, 2): p * cross, (1, 2): p * along, (2, 3): tp * cross, (2, 4): tp * along,
                0: cr, 1: ar, 2: p * rest, 3: t * cr, 4: t * ar,
            }
            sums = new if sums is None else {key: sums[key] + new[key] for key in new}
        sums[2, 2] = square[h]
        line = [sums[key] for key in sorted(sums, key=lambda key: PLACE[key])]
        groups = [fold_subs(line[i : i + SUBS], sub) for i in range(0, SUMS, SUBS)]
        groups += [jnp.zeros_like(groups[0])] * (ROWS // SUBS - len(groups))
        stacked.append(jnp.concatenate(groups, axis=0))
    for h, value in enumerate(stacked):
        for k, part in enumerate(split2(value)):
            at = (k * halves + h) * LANES
            packed[:, at : at + LANES] = part

    @pl.when(above > 0)
    def _():
        pl.semaphore_wait(met, above)

    normal = lax.dot_general(
        member[...], packed[...], (((1,), (1,)), ((), ())), preferred_element_type=jnp.float32
    )
    tiles[:, :, :ROWS] = normal.reshape(n_tm, owned, ROWS)

    for d in (*range(1, n_tm), 0):
        peer = lax.rem(tm + d, n_tm)
        pltpu.make_async_remote_copy(
            src_ref=tiles.at[peer],
            dst_ref=landed.at[d],
            send_sem=send_sem,
            recv_sem=sum_recv,
            device_id={"sky": mate, "tm": peer},
            device_id_type=MESH,
        ).start()
    prior_copy.wait()
    pltpu.make_async_copy(landed, landed, sum_recv).wait()
    terms = [landed[d] for d in range(n_tm)]
    while len(terms) > 1:
        odd = terms[len(terms) // 2 * 2 :]
        terms = [a + b for a, b in zip(terms[::2], terms[1::2])] + odd
    total = terms[0]
    flat[...] = jnp.transpose(total)[:ROWS]
    result = solve_rows(lambda i: flat[i : i + 1, :], lambda i: prior_ref[i : i + 1, :])
    for i in range(5):
        out_ref[i : i + 1, :] = result[i]
    pltpu.make_async_copy(landed, landed, send_sem).wait()


def on_device(n_sky, n_tm, attitude, time, parallax, observed, phase, knot, source, count, prior):
    slots, blocks, owned = time.shape[0], source.shape[0], prior.shape[1]
    knots = attitude.shape[2]
    rows = slots // LANES
    span = slots // blocks
    sources = owned * n_tm
    shape = (rows, LANES)
    vmem = pltpu.VMEM
    f32, i32, bf16 = jnp.float32, jnp.int32, jnp.bfloat16
    halves = (LANES // span) // (LANES // rows)
    return pl.pallas_call(
        functools.partial(kernel, n_sky, n_tm, span),
        out_shape=pltpu.VMEM(prior.shape, f32),
        in_specs=[pl.BlockSpec(memory_space=pl.ANY)] * 9,
        out_specs=pl.BlockSpec(memory_space=pltpu.VMEM),
        scratch_shapes=[
            vmem((4, knots), f32),
            vmem((n_sky, 4, knots), f32),
            vmem((4,) + shape, f32),
            vmem((rows + 2 * (blocks // LANES), LANES), i32),
            vmem(shape, i32),
            vmem(shape, i32),
            vmem((4,) + shape, f32),
            vmem((2, 4) + shape, f32),
            vmem((5,) + shape, f32),
            vmem((4,) + shape, f32),
            vmem((halves, SUBS, LANES), f32),
            vmem((sources, 2 * blocks), bf16),
            vmem((n_tm, owned, LANES), f32),
            vmem((n_tm, owned, LANES), f32),
        ]
        + [pltpu.SemaphoreType.DMA] * 3
        + [pltpu.SemaphoreType.DMA((2,))]
        + [pltpu.SemaphoreType.DMA((n_sky - 1,))]
        + [pltpu.SemaphoreType.DMA]
        + [pltpu.SemaphoreType.REGULAR]
        + [vmem((4,) + shape, f32), vmem((rows + 2 * (blocks // LANES), LANES), i32)]
        + [vmem(prior.shape, f32), vmem((ROWS, owned), f32), vmem((ROWS, 2 * blocks), bf16)],
        compiler_params=pltpu.CompilerParams(collective_id=0, has_side_effects=True),
    )(
        attitude.reshape(4, knots),
        time.reshape(shape),
        parallax.reshape(shape),
        observed.reshape(shape),
        phase.reshape(shape),
        knot.reshape(shape),
        source.reshape(blocks // LANES, LANES),
        count.reshape(blocks // LANES, LANES),
        prior,
    )


def solution(mesh):
    slot = P(("sky", "tm"))
    in_specs = (P(None, "tm", "sky"),) + (slot,) * 7 + (P(None, ("sky", "tm")),)
    return jax.shard_map(
        functools.partial(on_device, mesh.shape["sky"], mesh.shape["tm"]),
        mesh=mesh,
        in_specs=in_specs,
        out_specs=P(None, ("sky", "tm")),
        check_vma=False,
    )
```

```python
import functools

import jax
import jax.numpy as jnp
from jax import lax
from jax.experimental import pallas as pl
from jax.experimental.pallas import tpu as pltpu
from jax.sharding import PartitionSpec as P

PAIR_LIST = [(i, j) for i in range(5) for j in range(i, 5)]
MESH = pl.DeviceIdType.MESH
LANES = 128
SUBS = 8
ROWS = 32


def lane_gather(row, index):
    wide = jnp.broadcast_to(row, index.shape)
    return jnp.take_along_axis(wide, index, axis=1, mode="promise_in_bounds")


def split2(value):
    high = value.astype(jnp.bfloat16)
    return high, (value - high.astype(jnp.float32)).astype(jnp.bfloat16)


def solve_rows(row, prior_row):
    entry = {}
    for i, j in PAIR_LIST:
        entry[j, i] = row(PLACE[i, j])
    for i in range(5):
        entry[i, i] = entry[i, i] + prior_row(i)
    right = [row(PLACE[i]) for i in range(5)]
    unit, inverse = {}, []
    for col in range(5):
        inv = 1.0 / entry[col, col]
        inverse.append(inv)
        for r in range(col + 1, 5):
            unit[r, col] = entry[r, col] * inv
        for r in range(col + 1, 5):
            for c in range(col + 1, r + 1):
                entry[r, c] = entry[r, c] - unit[r, col] * entry[c, col]
            right[r] = right[r] - unit[r, col] * right[col]
    result = [right[i] * inverse[i] for i in range(5)]
    for i in range(4, 0, -1):
        for k in range(i):
            result[k] = result[k] - unit[i, k] * result[i]
    return result


PLACE = {
    (0, 0): 0, (0, 1): 1, (0, 3): 2, (0, 4): 3, (1, 3): 3, (1, 1): 4, (1, 4): 5, (3, 3): 6, (3, 4): 7,
    (4, 4): 8, (0, 2): 9, (1, 2): 10, (2, 3): 11, (2, 4): 12, 0: 13, 1: 14, 2: 15,
    3: 16, 4: 17, (2, 2): 18,
}
SUMS = 19


def orders(tm, n_tm):
    if n_tm % 2 == 0 and n_tm <= 8:

        def order(peer):
            up, across = peer // 2, peer % 2
            earlier = jnp.logical_and(tm // 2 >= up, tm % 2 >= across)
            later = jnp.logical_and(tm // 2 <= up, tm % 2 <= across)
            return jnp.logical_and(earlier, tm != peer), jnp.logical_and(later, tm != peer)
    else:

        def order(peer):
            return tm > peer, tm < peer

    return [(peer, *order(peer)) for peer in range(n_tm)]


def sky_peers(sky, n_sky):
    if n_sky & (n_sky - 1):
        sends = [(lax.rem(sky + d, n_sky), d - 1) for d in range(1, n_sky)]
        return sends, [(lax.rem(sky + n_sky - d, n_sky), d - 1) for d in range(1, n_sky)]
    core = sky % 2
    mate = sky + 1 - 2 * core
    sends, arrivals = [], [(mate, 0)]
    for k in range(1, n_sky // 2):
        base = sky - core
        for bit in [1 << i for i in range(1, n_sky.bit_length())]:
            if 2 * k & bit:
                base = base + bit * (1 - 2 * ((sky // bit) % 2))
        sends += [(base + 1, 2 * k - 1 + core), (base, 2 * k - 1 + core)]
        arrivals += [(base + 1, 2 * k), (base, 2 * k - 1)]
    return sends + [(mate, 0)], arrivals


def tell(semaphore, sky, peer, exists):
    @pl.when(exists)
    def _():
        there = {"sky": sky, "tm": peer}
        pl.semaphore_signal(semaphore, inc=1, device_id=there, device_id_type=MESH)


def fold_subs(values, sub):
    values = list(values) + [jnp.zeros_like(values[0])] * (SUBS - len(values))
    values = [values[i] for i in (0, 4, 2, 6, 1, 5, 3, 7)]
    step = 1
    while step < SUBS:
        low = (sub // step) % 2 == 0
        half = len(values) // 2
        values = [
            jnp.where(low, a, b) + pltpu.roll(jnp.where(low, b, a), step, 0)
            for a, b in zip(values[:half], values[half:])
        ]
        step *= 2
    return values[0]


def kernel(
    n_sky, n_tm, span,
    attitude_hbm, time_hbm, parallax_hbm, observed_hbm, phase_hbm, knot_hbm,
    source_hbm, count_hbm, prior_hbm,
    out_ref,
    mine, table, reals, ints, low, high, weight, masked, fact, quat, square, member, tiles, landed,
    real_sem, int_sem, send_sem, slot_recv, att_recv, sum_recv, met, got_reals, got_ints, prior_ref, flat, packed,
):
    own = pltpu.make_async_copy(attitude_hbm, mine, send_sem)
    own.start()
    sky = lax.axis_index("sky")
    tm = lax.axis_index("tm")
    rows = time_hbm.shape[0]
    owned = tiles.shape[1]
    wide = source_hbm.shape[0]
    phase_v, time_v, parallax_v, observed_v = (reals.at[i] for i in range(4))
    knot_v = ints.at[:rows]
    source_v = ints.at[rows : rows + wide]
    count_v = ints.at[rows + wide :]
    sources = owned * n_tm
    segs = LANES // span
    fold = LANES // rows
    halves = segs // fold
    steps = span // SUBS

    barrier = pltpu.get_barrier_semaphore()
    sends, arrivals = sky_peers(sky, n_sky)
    for peer, _ in sends:
        pl.semaphore_signal(barrier, inc=1, device_id={"sky": peer}, device_id_type=MESH)
    for src, dst in ((source_hbm, source_v), (count_hbm, count_v), (knot_hbm, knot_v)):
        pltpu.make_async_copy(src, dst, int_sem).start()
    for i, src in enumerate((phase_hbm, time_hbm, parallax_hbm, observed_hbm)):
        pltpu.make_async_copy(src, reals.at[i], real_sem).start()
    peers = orders(tm, n_tm)
    below = sum(earlier.astype(jnp.int32) for _, earlier, _ in peers)
    above = sum(later.astype(jnp.int32) for _, _, later in peers)
    mate = sky + 1 - 2 * (sky % 2)
    for peer, _, later in peers:
        tell(barrier, sky, peer, later)
        tell(barrier, mate, peer, later)

    tiles[...] = jnp.zeros_like(tiles)

    own.wait()
    pl.semaphore_wait(barrier, n_sky - 1 + 2 * below)
    for peer, there in sends:
        pltpu.make_async_remote_copy(
            src_ref=mine,
            dst_ref=table.at[sky],
            send_sem=send_sem,
            recv_sem=att_recv.at[there],
            device_id={"sky": peer},
            device_id_type=MESH,
        ).start()
    loaded = ((ints, got_ints, int_sem), (reals, got_reals, real_sem))
    for k, (here, there, semaphore) in enumerate(loaded):
        pltpu.make_async_copy(here, here, semaphore).wait()
        pltpu.make_async_remote_copy(
            src_ref=here,
            dst_ref=there,
            send_sem=semaphore,
            recv_sem=slot_recv.at[k],
            device_id={"sky": mate},
            device_id_type=MESH,
        ).start()
    for peer, earlier, _ in peers:
        tell(met, mate, peer, earlier)

    pltpu.make_async_copy(got_ints, got_ints, slot_recv.at[0]).wait()
    lane = lax.broadcasted_iota(jnp.int32, (SUBS, LANES), 1)
    sub = lax.broadcasted_iota(jnp.int32, (SUBS, LANES), 0)
    count = []
    which = lax.broadcasted_iota(jnp.int32, (sources, LANES), 0)
    for h in range(halves):
        block = (lane % rows) * segs + h * fold + lane // rows

        def of_block(ref):
            got = lane_gather(ref[0:1, :], block % LANES)
            for c in range(1, wide):
                got = jnp.where(block // LANES == c, lane_gather(ref[c : c + 1, :], block % LANES), got)
            return got

        count.append(of_block(got_ints.at[rows + wide :]))
        hit = jnp.broadcast_to(of_block(got_ints.at[rows : rows + wide])[0:1, :], (sources, LANES)) == which
        one = jnp.where(hit, 1.0, 0.0).astype(jnp.bfloat16)
        for k in range(2):
            at = (k * halves + h) * LANES
            member[:, at : at + LANES] = one

    def turn(value):
        parts = [value] + [pltpu.roll(value, LANES - e * span, 1) for e in range(1, fold)]
        turned = jnp.transpose(jnp.concatenate(parts, axis=0))
        return [turned[h * fold * span : h * fold * span + span, :] for h in range(halves)]

    for h, knot in enumerate(turn(got_ints[:rows, :])):
        at = slice(h * span, h * span + span)
        low[at, :] = knot % LANES
        high[at, :] = knot // LANES

    pltpu.make_async_copy(got_reals, got_reals, slot_recv.at[1]).wait()
    turned = [turn(got_reals[i]) for i in range(4)]
    for h in range(halves):
        at = slice(h * span, h * span + span)
        u, time, parallax, observed = (t[h] for t in turned)
        slot = lax.broadcasted_iota(jnp.int32, (span, LANES), 0)
        live = slot < jnp.broadcast_to(count[h][0:1, :], (span, LANES))
        u2, v = u * u, 1.0 - u
        u3 = u2 * u
        spline = (
            v * v * v * (1.0 / 6.0),
            0.5 * u3 - u2 + (2.0 / 3.0),
            0.5 * (u + u2 - u3) + (1.0 / 6.0),
            u3 * (1.0 / 6.0),
        )
        for i in range(4):
            weight[i, at, :] = jnp.where(live, spline[i], 0.0)
        parallax = jnp.where(live, parallax, 0.0)
        fact[0, at, :] = time
        fact[1, at, :] = time * time
        fact[2, at, :] = parallax
        fact[3, at, :] = parallax * time
        fact[4, at, :] = observed
        both = parallax * parallax
        total = both[:SUBS]
        for g in range(1, steps):
            total = total + both[g * SUBS : (g + 1) * SUBS]
        square[h] = total

    per = table.shape[2] // LANES

    def mask_weights(slot, chunk):
        lows, highs = low[...], high[...]
        for i in range(4):
            there = highs + (lows >= LANES - i).astype(jnp.int32) if i else highs
            masked[slot, i] = jnp.where(there == chunk, weight[i], 0.0)

    def rows_of(source, p, first):
        at = slice(p * LANES, (p + 1) * LANES)
        here = mine[:, at] if first else table[source, :, at]
        return [here] + [pltpu.roll(here, LANES - i, 1) for i in range(1, 4)]

    def gather(group, v, carry):
        at = slice(v * SUBS, v * SUBS + SUBS)
        index = low[at, :]
        got = list(carry) if carry else [None] * 4
        for slot, shifted in enumerate(group):
            for i in range(4):
                scale = masked[slot, i, at, :]
                for m in range(4):
                    term = lane_gather(shifted[i][m : m + 1, :], index) * scale
                    got[m] = term if got[m] is None else got[m] + term
        return got

    pieces = [(sky, None, p, True) for p in range(per)]
    for source, here in arrivals:
        pieces += [(source, here if p == 0 else None, p, False) for p in range(per)]
    ahead = 2 if len(pieces) > 2 else 1
    groups = [pieces[:ahead]] + [[piece] for piece in pieces[ahead:]]
    for n, group in enumerate(groups):
        for slot, (source, here, p, first) in enumerate(group):
            mask_weights(slot, source * per + p)
        if n + 1 == len(groups):
            others = table.at[: n_sky - 1]
            pltpu.make_async_copy(others, others, send_sem).wait()
            pltpu.make_async_copy(ints, ints, int_sem).wait()
            pltpu.make_async_copy(reals, reals, real_sem).wait()
            prior_copy = pltpu.make_async_copy(prior_hbm, prior_ref, int_sem)
            prior_copy.start()
        for source, here, p, first in group:
            if here is not None:
                arrived = table.at[source]
                pltpu.make_async_copy(arrived, arrived, att_recv.at[here]).wait()
        shifted = [rows_of(source, p, first) for source, here, p, first in group]
        if n + 1 < len(groups):
            for v in range(rows // SUBS):
                at = slice(v * SUBS, v * SUBS + SUBS)
                got = gather(shifted, v, [quat[m, at, :] for m in range(4)] if n else None)
                for m in range(4):
                    quat[m, at, :] = got[m]

    stacked = []
    for h in range(halves):
        sums = None
        for g in range(steps):
            v = h * steps + g
            at = slice(v * SUBS, v * SUBS + SUBS)
            carry = [quat[m, at, :] for m in range(4)] if len(groups) > 1 else None
            q0, q1, q2, q3 = gather(shifted, v, carry)
            cross = (q0 * q0 + q1 * q1) - (q2 * q2 + q3 * q3)
            along = 2.0 * (q1 * q2 + q0 * q3)
            tilt = 2.0 * (q1 * q3 - q0 * q2)
            t, tt, p, tp, o = (fact[i, at, :] for i in range(5))
            rest = o - tilt
            cc, ca, aa = cross * cross, cross * along, along * along
            cr, ar = cross * rest, along * rest
            new = {
                (0, 0): cc, (0, 1): ca, (0, 3): t * cc, (0, 4): t * ca, (1, 1): aa, (1, 4): t * aa,
                (3, 3): tt * cc, (3, 4): tt * ca, (4, 4): tt * aa,
                (0, 2): p * cross, (1, 2): p * along, (2, 3): tp * cross, (2, 4): tp * along,
                0: cr, 1: ar, 2: p * rest, 3: t * cr, 4: t * ar,
            }
            sums = new if sums is None else {key: sums[key] + new[key] for key in new}
        sums[2, 2] = square[h]
        line = [sums[key] for key in sorted(sums, key=lambda key: PLACE[key])]
        groups = [fold_subs(line[i : i + SUBS], sub) for i in range(0, SUMS, SUBS)]
        groups += [jnp.zeros_like(groups[0])] * (ROWS // SUBS - len(groups))
        stacked.append(jnp.concatenate(groups, axis=0))
    for h, value in enumerate(stacked):
        for k, part in enumerate(split2(value)):
            at = (k * halves + h) * LANES
            packed[:, at : at + LANES] = part

    @pl.when(above > 0)
    def _():
        pl.semaphore_wait(met, above)

    normal = lax.dot_general(
        member[...], packed[...], (((1,), (1,)), ((), ())), preferred_element_type=jnp.float32
    )
    tiles[:, :, :ROWS] = normal.reshape(n_tm, owned, ROWS)

    for d in (*range(1, n_tm), 0):
        peer = lax.rem(tm + d, n_tm)
        pltpu.make_async_remote_copy(
            src_ref=tiles.at[peer],
            dst_ref=landed.at[d],
            send_sem=send_sem,
            recv_sem=sum_recv,
            device_id={"sky": mate, "tm": peer},
            device_id_type=MESH,
        ).start()
    prior_copy.wait()
    pltpu.make_async_copy(landed, landed, sum_recv).wait()
    terms = [landed[d] for d in range(n_tm)]
    while len(terms) > 1:
        odd = terms[len(terms) // 2 * 2 :]
        terms = [a + b for a, b in zip(terms[::2], terms[1::2])] + odd
    total = terms[0]
    flat[...] = jnp.transpose(total)[:ROWS]
    result = solve_rows(lambda i: flat[i : i + 1, :], lambda i: prior_ref[i : i + 1, :])
    for i in range(5):
        out_ref[i : i + 1, :] = result[i]
    pltpu.make_async_copy(landed, landed, send_sem).wait()


def on_device(n_sky, n_tm, attitude, time, parallax, observed, phase, knot, source, count, prior):
    slots, blocks, owned = time.shape[0], source.shape[0], prior.shape[1]
    knots = attitude.shape[2]
    rows = slots // LANES
    span = slots // blocks
    sources = owned * n_tm
    shape = (rows, LANES)
    vmem = pltpu.VMEM
    f32, i32, bf16 = jnp.float32, jnp.int32, jnp.bfloat16
    halves = (LANES // span) // (LANES // rows)
    return pl.pallas_call(
        functools.partial(kernel, n_sky, n_tm, span),
        out_shape=pltpu.VMEM(prior.shape, f32),
        in_specs=[pl.BlockSpec(memory_space=pl.ANY)] * 9,
        out_specs=pl.BlockSpec(memory_space=pltpu.VMEM),
        scratch_shapes=[
            vmem((4, knots), f32),
            vmem((n_sky, 4, knots), f32),
            vmem((4,) + shape, f32),
            vmem((rows + 2 * (blocks // LANES), LANES), i32),
            vmem(shape, i32),
            vmem(shape, i32),
            vmem((4,) + shape, f32),
            vmem((2, 4) + shape, f32),
            vmem((5,) + shape, f32),
            vmem((4,) + shape, f32),
            vmem((halves, SUBS, LANES), f32),
            vmem((sources, 2 * blocks), bf16),
            vmem((n_tm, owned, LANES), f32),
            vmem((n_tm, owned, LANES), f32),
        ]
        + [pltpu.SemaphoreType.DMA] * 3
        + [pltpu.SemaphoreType.DMA((2,))]
        + [pltpu.SemaphoreType.DMA((n_sky - 1,))]
        + [pltpu.SemaphoreType.DMA]
        + [pltpu.SemaphoreType.REGULAR]
        + [vmem((4,) + shape, f32), vmem((rows + 2 * (blocks // LANES), LANES), i32)]
        + [vmem(prior.shape, f32), vmem((ROWS, owned), f32), vmem((ROWS, 2 * blocks), bf16)],
        compiler_params=pltpu.CompilerParams(collective_id=0, has_side_effects=True),
    )(
        attitude.reshape(4, knots),
        time.reshape(shape),
        parallax.reshape(shape),
        observed.reshape(shape),
        phase.reshape(shape),
        knot.reshape(shape),
        source.reshape(blocks // LANES, LANES),
        count.reshape(blocks // LANES, LANES),
        prior,
    )


def solution(mesh):
    slot = P(("sky", "tm"))
    in_specs = (P(None, "tm", "sky"),) + (slot,) * 7 + (P(None, ("sky", "tm")),)
    return jax.shard_map(
        functools.partial(on_device, mesh.shape["sky"], mesh.shape["tm"]),
        mesh=mesh,
        in_specs=in_specs,
        out_specs=P(None, ("sky", "tm")),
        check_vma=False,
    )
```
